8 devices in a mesh: model: 8 (over z, y, x, core).
Axes of the slice: x: 2, y: 2, z: 1, core: 2. Of those that a mesh axis runs over, the one named last changes fastest.
Arguments:
- act_in: bfloat16 [4096, 4096], P('model')
- ln_gain: float32 [4096], replicated
- w_q: bfloat16 [4096, 4096], P(None, 'model')
- w_kv: bfloat16 [4096, 512], replicated
- w_o: bfloat16 [4096, 4096], P('model')
- positions: int32 [4096], replicated
Outputs:
- output 1: bfloat16 [4096, 4096], P('model')
- output 2: bfloat16 [4096, 256], replicated
- output 3: bfloat16 [4096, 256], replicated
All inputs are finite; a program needn't handle non-finite values.
Results may differ from the reference program's by a relative error of at most 0.0117956.
Values are sent between devices in bfloat16 or wider.
A program may use at most 1 GiB of HBM per device.

```python
import jax
import jax.numpy as jnp
from jax import lax

TOKENS = 4096
SEQ = 4096
D = 4096
HEADS = 16
HEAD = 256
NORM_EPS = 1e-6


def setup_inputs(seed: int = 0) -> dict:
    rng_keys = jax.random.split(jax.random.key(seed), 6)
    act_in = jax.random.normal(rng_keys[0], (TOKENS, D), jnp.float32).astype(jnp.bfloat16)
    ln_gain = jax.random.uniform(rng_keys[1], (D,), jnp.float32, 0.6, 1.4)
    w_q = (jax.random.normal(rng_keys[2], (D, HEADS * HEAD), jnp.float32) * D ** -0.5).astype(jnp.bfloat16)
    w_kv = (jax.random.normal(rng_keys[3], (D, 2 * HEAD), jnp.float32) * D ** -0.5).astype(jnp.bfloat16)
    out_scale = (SEQ / (HEADS * HEAD)) ** 0.5 / 8.0
    w_o = (jax.random.normal(rng_keys[4], (HEADS * HEAD, D), jnp.float32) * out_scale).astype(jnp.bfloat16)
    positions = jax.random.permutation(rng_keys[5], SEQ).astype(jnp.int32)
    return dict(act_in=act_in, ln_gain=ln_gain, w_q=w_q, w_kv=w_kv, w_o=w_o, positions=positions)


def layer_norm(act_rows, gain_vec):
    rows_f32 = act_rows.astype(jnp.float32)
    row_mean = jnp.mean(rows_f32, axis=-1, keepdims=True)
    centered = rows_f32 - row_mean
    variance = jnp.mean(centered * centered, axis=-1, keepdims=True)
    return (centered * lax.rsqrt(variance + NORM_EPS) * gain_vec).astype(jnp.bfloat16)


def reference(act_in, ln_gain, w_q, w_kv, w_o, positions):
    normed = layer_norm(act_in, ln_gain)
    queries = jnp.dot(normed, w_q, preferred_element_type=jnp.float32).astype(jnp.bfloat16)
    kv_proj = jnp.dot(normed, w_kv, preferred_element_type=jnp.float32).astype(jnp.bfloat16)
    k_cache = kv_proj[:, :HEAD]
    v_cache = kv_proj[:, HEAD:]
    n_seq = TOKENS // SEQ
    visible = positions[None, :] <= positions[:, None]
    q_seqs = queries.reshape(n_seq, SEQ, HEADS, HEAD).transpose(0, 2, 1, 3)
    k_seqs = k_cache.reshape(n_seq, SEQ, HEAD)
    v_seqs = v_cache.reshape(n_seq, SEQ, HEAD)

    def one_seq(operands):
        q_blk, k_blk, v_blk = operands

        def one_head(q_head):
            scores = jnp.dot(q_head, k_blk.T, preferred_element_type=jnp.float32) * HEAD ** -0.5
            scores = jnp.where(visible, scores, -1e30)
            attn_prob = jax.nn.softmax(scores, axis=-1).astype(jnp.bfloat16)
            return jnp.dot(attn_prob, v_blk, preferred_element_type=jnp.float32).astype(jnp.bfloat16)

        return lax.map(one_head, q_blk)

    attended = lax.map(one_seq, (q_seqs, k_seqs, v_seqs))
    attended = attended.transpose(0, 2, 1, 3).reshape(TOKENS, HEADS * HEAD)
    y_out = jnp.dot(attended, w_o, preferred_element_type=jnp.float32).astype(jnp.bfloat16)
    return y_out, k_cache, v_cache
```

```python
import functools
import math

import jax
import jax.numpy as jnp
from jax import lax
from jax.experimental import pallas as pl
from jax.experimental.pallas import tpu as pltpu
from jax.sharding import PartitionSpec as P

NORM_EPS = 1e-6
NEG = -1e30
F32 = jnp.float32
BF16 = jnp.bfloat16
ANY = pl.BlockSpec(memory_space=pl.ANY)
VMEM_LIMIT = 56 * 1024 * 1024


def cost(flops, nbytes):
    return pl.CostEstimate(flops=int(flops), bytes_accessed=int(nbytes), transcendentals=0)


def params(n):
    return pltpu.CompilerParams(dimension_semantics=("arbitrary",) * n, vmem_limit_bytes=VMEM_LIMIT)


def normalize(rows, gain):
    rows = rows.astype(F32)
    width = rows.shape[-1]
    mean = jnp.sum(rows, axis=-1, keepdims=True) * (1.0 / width)
    centered = rows - mean
    var = jnp.sum(centered * centered, axis=-1, keepdims=True) * (1.0 / width)
    return (centered * lax.rsqrt(var + NORM_EPS) * gain).astype(BF16)


def norm_kv_kernel(x_ref, g_ref, w_ref, h_ref, kv_ref):
    h = normalize(x_ref[...], g_ref[...])
    h_ref[...] = h
    kv_ref[...] = jnp.dot(h, w_ref[...], preferred_element_type=F32).astype(BF16)


def norm_kv(x, g, w_kv, block=128):
    rows, width = x.shape
    n = w_kv.shape[1]
    return pl.pallas_call(
        norm_kv_kernel,
        grid=(rows // block,),
        in_specs=[
            pl.BlockSpec((block, width), lambda i: (i, 0)),
            pl.BlockSpec((1, width), lambda i: (0, 0)),
            pl.BlockSpec((width, n), lambda i: (0, 0)),
        ],
        out_specs=[
            pl.BlockSpec((block, width), lambda i: (i, 0)),
            pl.BlockSpec((block, n), lambda i: (i, 0)),
        ],
        out_shape=[jax.ShapeDtypeStruct((rows, width), BF16), jax.ShapeDtypeStruct((rows, n), BF16)],
        compiler_params=params(1),
        cost_estimate=cost(2 * rows * width * n, 4 * rows * width + 2 * width * n),
        name="norm_kv",
    )(x, g, w_kv)


def norm_kernel(x_ref, g_ref, h_ref):
    h_ref[...] = normalize(x_ref[...], g_ref[...])


def norm(x, g, block=64):
    rows, width = x.shape
    return pl.pallas_call(
        norm_kernel,
        grid=(rows // block,),
        in_specs=[
            pl.BlockSpec((block, width), lambda i: (i, 0)),
            pl.BlockSpec((1, width), lambda i: (0, 0)),
        ],
        out_specs=pl.BlockSpec((block, width), lambda i: (i, 0)),
        out_shape=jax.ShapeDtypeStruct((rows, width), BF16),
        compiler_params=params(1),
        cost_estimate=cost(rows * width * 1000, 4 * rows * width),
        name="norm",
    )(x, g)


def attend_kernel(chunk, h_ref, w_ref, kt_ref, v_ref, pq_ref, pk_ref, _, o_ref, s_ref):
    q = jnp.dot(h_ref[...], w_ref[...], preferred_element_type=F32).astype(BF16)
    rows, depth = q.shape
    keys = kt_ref.shape[1]
    lanes = pq_ref.shape[1]
    factor = depth ** -0.5 * math.log2(math.e)
    row_pos = pq_ref[...]
    top = None
    for j in range(keys // chunk):
        cols = slice(j * chunk, (j + 1) * chunk)
        s = jnp.dot(q, kt_ref[:, cols], preferred_element_type=F32)
        for i in range(chunk // lanes):
            lo = j * chunk + i * lanes
            seen = pk_ref[:, lo : lo + lanes] <= row_pos
            part = jnp.where(seen, s[:, i * lanes : (i + 1) * lanes], NEG)
            s_ref[:, lo : lo + lanes] = part
            top = part if top is None else jnp.maximum(top, part)
    top = jnp.max(top, axis=1, keepdims=True)
    total = None
    acc = None
    for j in range(keys // chunk):
        cols = slice(j * chunk, (j + 1) * chunk)
        p = jnp.exp2((s_ref[:, cols] - top) * factor)
        for i in range(chunk // lanes):
            part = p[:, i * lanes : (i + 1) * lanes]
            total = part if total is None else total + part
        pv = jnp.dot(p.astype(BF16), v_ref[cols, :], preferred_element_type=F32)
        acc = pv if acc is None else acc + pv
    total = jnp.sum(total, axis=1, keepdims=True)
    o_ref[...] = (acc * (1.0 / total)).astype(BF16)


def attend(out, row0, col0, h, w, kt, v, row_pos, key_pos, block=256, chunk=512):
    rows, width = h.shape
    depth, keys = kt.shape
    heads = w.shape[1] // depth
    block = min(block, rows)
    lanes = row_pos.shape[1]
    r0, c0 = row0 // block, col0 // depth
    in_specs = [
        pl.BlockSpec((block, width), lambda n, i: (i, 0)),
        pl.BlockSpec((width, depth), lambda n, i: (0, n)),
        pl.BlockSpec((depth, keys), lambda n, i: (0, 0)),
        pl.BlockSpec((keys, depth), lambda n, i: (0, 0)),
        pl.BlockSpec((block, lanes), lambda n, i: (i, 0)),
        pl.BlockSpec((1, keys), lambda n, i: (0, 0)),
        ANY,
    ]
    return pl.pallas_call(
        functools.partial(attend_kernel, chunk),
        grid=(heads, rows // block),
        in_specs=in_specs,
        out_specs=pl.BlockSpec((block, depth), lambda n, i: (r0 + i, c0 + n)),
        out_shape=jax.ShapeDtypeStruct(out.shape, BF16),
        scratch_shapes=[pltpu.VMEM((block, keys), F32)],
        input_output_aliases={6: 0},
        compiler_params=params(2),
        cost_estimate=cost(2 * rows * depth * heads * (width + 2 * keys), 2 * width * depth * heads + 2 * rows * width + 4 * keys * depth),
        name="attend",
    )(h, w, kt, v, row_pos, key_pos, out)


def project_kernel(n, *refs):
    o_ref, w_refs, y_ref = refs[0], refs[1 : 1 + n], refs[-1]
    acc = None
    depth = w_refs[0].shape[0]
    for i in range(n):
        part = jnp.dot(o_ref[:, i * depth : (i + 1) * depth], w_refs[i][...], preferred_element_type=F32)
        acc = part if acc is None else acc + part
    if len(refs) > n + 2:
        acc = acc + refs[1 + n][...].astype(F32)
    y_ref[...] = acc.astype(BF16)


def project(o, ws, cols, width, other=None, y=None, block=512):
    rows, total = o.shape
    n = len(ws)
    depth = total // n
    block = min(block, width)
    in_specs = [pl.BlockSpec((rows, total), lambda i: (0, 0))]
    for w, start in ws:
        off = (cols - start) // block
        in_specs.append(pl.BlockSpec((depth, block), lambda i, off=off: (0, off + i)))
    args = [o] + [w for w, _ in ws]
    aliases = {}
    if other is None:
        out_shape = jax.ShapeDtypeStruct((rows, width), BF16)
        out_spec = pl.BlockSpec((rows, block), lambda i: (0, i))
    else:
        in_specs.append(pl.BlockSpec((rows, block), lambda i: (0, i)))
        args.append(other)
        c0 = cols // block
        out_shape = jax.ShapeDtypeStruct(y.shape, BF16)
        out_spec = pl.BlockSpec((rows, block), lambda i: (0, c0 + i))
        in_specs.append(ANY)
        args.append(y)
        aliases = {len(args) - 1: 0}
    return pl.pallas_call(
        functools.partial(project_kernel, n),
        grid=(width // block,),
        in_specs=in_specs,
        out_specs=out_spec,
        out_shape=out_shape,
        input_output_aliases=aliases,
        compiler_params=params(1),
        cost_estimate=cost(2 * rows * total * width, 2 * rows * total + 2 * total * width + 2 * rows * width),
        name="project",
    )(*args)


def solution(mesh):
    count = mesh.shape["model"]
    side = [(d, d ^ 1) for d in range(count)]
    along_x = [(d, d ^ 2) for d in range(count)]
    along_y = [(d, d ^ 4) for d in range(count)]

    def hop(value, pairs, name):
        with jax.named_scope(name):
            return lax.ppermute(value, "model", pairs)

    def after(value, *deps):
        return lax.optimization_barrier((value, *deps))[0]

    def local_step(x_loc, ln_gain, wq_loc, w_kv, wo_loc, positions):
        me = lax.axis_index("model")
        rows, width = x_loc.shape
        seq_len = positions.shape[0]
        depth = w_kv.shape[1] // 2
        heads2 = wq_loc.shape[1]
        gain = ln_gain.reshape(1, width)

        x_cut = (0, 64, 256, 384, 512)
        x_parts = [x_loc[a:b] for a, b in zip(x_cut, x_cut[1:])]
        wo_cut = (0, 512, 1024, 2048, 3072, 4096)
        wo_parts = [wo_loc[:, a:b] for a, b in zip(wo_cut, wo_cut[1:])]
        x_got = [hop(x_parts[0], along_x, "x0")]
        wo_got = [hop(wo_parts[0], along_y, "wo0")]
        wq_side = hop(wq_loc, side, "wq_side")
        wo_side = hop(wo_loc, side, "wo_side")

        h_own, kv_own = norm_kv(x_loc, gain, w_kv)

        kv_x = hop(kv_own, along_x, "kv_x")
        kv_y = hop(kv_own, along_y, "kv_y")
        kv_d = hop(kv_x, along_y, "kv_d")
        kv_s0 = hop(jnp.concatenate([kv_own, kv_x], 0), side, "kv_s0")
        kv_s1 = hop(jnp.concatenate([kv_y, kv_d], 0), side, "kv_s1")
        blocks = jnp.concatenate([kv_own, kv_x, kv_y, kv_d, kv_s0, kv_s1], 0).reshape(count, rows, 2 * depth)
        order = jnp.array([0, 4, 1, 5, 2, 6, 3, 7])
        place = order[jnp.arange(count) ^ me]
        kv_all = jnp.take(blocks, place, axis=0).reshape(count * rows, 2 * depth)
        k_all, v_all = kv_all[:, :depth], kv_all[:, depth:]
        kt_all = k_all.T

        for i in range(1, 4):
            x_got.append(hop(after(x_parts[i], kv_own), along_x, f"x{i}"))
        wq_a = hop(after(wq_loc[:, :depth], kv_x), along_y, "wq_a")
        wq_b = hop(after(wq_loc[:, depth:], kv_x), along_y, "wq_b")
        wq_as = hop(wq_a, side, "wq_as")
        wq_bs = hop(wq_b, side, "wq_bs")
        for i in range(1, 5):
            wo_got.append(hop(after(wo_parts[i], kv_d), along_y, f"wo{i}"))
        wo_gots = [hop(w, side, f"wo_s{i}") for i, w in enumerate(wo_got)]

        def positions_of(device):
            mine = lax.dynamic_slice(positions, (device * rows,), (rows,))
            return jnp.broadcast_to(mine[:, None], (rows, 128))

        pos_own, pos_other = positions_of(me), positions_of(me ^ 2)
        key_pos = positions.reshape(1, seq_len)

        o_own = jnp.zeros((rows, 4 * heads2), BF16)
        o_other = jnp.zeros((rows, 4 * heads2), BF16)
        run = functools.partial(attend, kt=kt_all, v=v_all, key_pos=key_pos)

        o_own = run(o_own, 0, 0, h_own, wq_loc, row_pos=pos_own)
        o_own = run(o_own, 0, heads2, h_own, wq_side, row_pos=pos_own)

        h0 = norm(jnp.concatenate(x_got[:2], 0), gain)
        p0 = pos_other[:256]
        o_other = run(o_other, 0, 0, h0, wq_loc, row_pos=p0)
        o_other = run(o_other, 0, heads2, h0, wq_side, row_pos=p0)
        o_own = run(o_own, 0, 2 * heads2, h_own, wq_a, row_pos=pos_own)
        o_own = run(o_own, 0, 3 * heads2, h_own, wq_as, row_pos=pos_own)
        o_other = run(o_other, 0, 2 * heads2, h0, wq_a, row_pos=p0)
        o_other = run(o_other, 0, 3 * heads2, h0, wq_as, row_pos=p0)
        for i in (2, 3):
            a, b = x_cut[i], x_cut[i + 1]
            hi = norm(x_got[i], gain)
            pi = pos_other[a:b]
            o_other = run(o_other, a, 0, hi, wq_loc, row_pos=pi)
            o_other = run(o_other, a, heads2, hi, wq_side, row_pos=pi)
            o_other = run(o_other, a, 2 * heads2, hi, wq_a, row_pos=pi)
            o_other = run(o_other, a, 3 * heads2, hi, wq_as, row_pos=pi)
            o_other = run(o_other, a, 2 * heads2 + depth, hi, wq_b, row_pos=pi)
            o_other = run(o_other, a, 3 * heads2 + depth, hi, wq_bs, row_pos=pi)
        o_other = run(o_other, 0, 2 * heads2 + depth, h0, wq_b, row_pos=p0)
        o_other = run(o_other, 0, 3 * heads2 + depth, h0, wq_bs, row_pos=p0)
        o_own = run(after(o_own, o_other), 0, 2 * heads2 + depth, h_own, wq_b, row_pos=pos_own)
        o_own = run(o_own, 0, 3 * heads2 + depth, h_own, wq_bs, row_pos=pos_own)

        y_got = []
        for i in range(5):
            a, b = wo_cut[i], wo_cut[i + 1]
            ws = [(wo_loc, 0), (wo_side, 0), (wo_got[i], a), (wo_gots[i], a)]
            y_got.append(hop(project(o_other, ws, a, b - a), along_x, f"y{i}"))
        y = jnp.zeros((rows, width), BF16)
        for i in range(5):
            a, b = wo_cut[i], wo_cut[i + 1]
            ws = [(wo_loc, 0), (wo_side, 0), (wo_got[i], a), (wo_gots[i], a)]
            y = project(o_own, ws, a, b - a, y_got[i], y)
        return y, k_all, v_all

    return jax.shard_map(
        local_step,
        mesh=mesh,
        in_specs=(P("model", None), P(None), P(None, "model"), P(None, None), P("model", None), P(None)),
        out_specs=(P("model", None), P(None, None), P(None, None)),
        check_vma=False,
    )
```

```python
import functools
import math

import jax
import jax.numpy as jnp
from jax import lax
from jax.experimental import pallas as pl
from jax.experimental.pallas import tpu as pltpu
from jax.sharding import PartitionSpec as P

NORM_EPS = 1e-6
NEG = -1e30
F32 = jnp.float32
BF16 = jnp.bfloat16
MESH = pl.DeviceIdType.MESH
VMEM_LIMIT = 67_000_000

BLOCK = 256
KEYS = 1024
X_CUT = (0, 64, 256, 384, 512)
A_CUT = 1024


class Copies:
    def __init__(self, send, recv):
        self.send, self.recv, self.used = send, recv, 0

    def take(self, n=1):
        first = self.used
        self.used += n
        return first

    def make(self, src, dst, i, peer):
        return pltpu.make_async_remote_copy(
            src_ref=src, dst_ref=dst, send_sem=self.send.at[i], recv_sem=self.recv.at[i], device_id=(peer,), device_id_type=MESH
        )


N_COPIES = 57


def kernel(
    x_hbm, wq_hbm, wkv_hbm, wo_hbm, gain_ref, pq_ref, pk_ref,
    y_hbm, k_hbm, v_hbm,
    h, kbuf, vbuf, wq, wo, o, s, ysend, yrecv, yout,
    send, recv, local, out_sem,
):
    me = lax.axis_index("model")
    rows = x_hbm.shape[0]
    width = x_hbm.shape[1]
    depth = kbuf.shape[1]
    keys = kbuf.shape[0]
    pieces = wo.shape[1]
    part = width // pieces
    slots = ysend.shape[0]

    def flip(bit):
        return me + bit - 2 * bit * lax.rem(lax.div(me, bit), 2)

    side, over_x, over_y = flip(1), flip(2), flip(4)
    over_d = over_x + over_y - me
    copies = Copies(send, recv)

    half = rows // 2
    load_x = [pltpu.make_async_copy(x_hbm.at[i * half : (i + 1) * half], h.at[i * half : (i + 1) * half], local.at[i]) for i in range(2)]
    quarter = width // 4
    load_kv = [
        pltpu.make_async_copy(wkv_hbm.at[j * quarter : (j + 1) * quarter], o.at[:, j * 2 * depth : (j + 1) * 2 * depth], local.at[2 + j])
        for j in range(4)
    ]
    load_wq = [pltpu.make_async_copy(wq_hbm.at[:, i * depth : (i + 1) * depth], wq.at[i], local.at[6 + i]) for i in range(2)]
    for copy in load_x + load_kv:
        copy.start()

    barrier = pltpu.get_barrier_semaphore()
    for peer in (side, over_x, over_y):
        pl.semaphore_signal(barrier, inc=1, device_id=(peer,), device_id_type=MESH)
    pl.semaphore_wait(barrier, 3)

    send_x = []
    for a, b in zip(X_CUT, X_CUT[1:]):
        send_x.append(copies.make(x_hbm.at[a:b], h.at[rows + a : rows + b], copies.take(), over_x))
    send_a0 = copies.make(wq_hbm.at[0:A_CUT, 0:depth], wq.at[4, 0:A_CUT], copies.take(), over_y)
    send_a1 = copies.make(wq_hbm.at[A_CUT:width, 0:depth], wq.at[4, A_CUT:width], copies.take(), over_y)
    send_b = copies.make(wq_hbm.at[:, depth : 2 * depth], wq.at[5], copies.take(), over_y)
    send_s = [copies.make(wq_hbm.at[:, i * depth : (i + 1) * depth], wq.at[2 + i], copies.take(), side) for i in range(2)]
    pass_a = copies.make(wq.at[4], wq.at[6], copies.take(), side)
    pass_b = copies.make(wq.at[5], wq.at[7], copies.take(), side)

    def block(buf, owner):
        return buf.at[pl.ds(pl.multiple_of(owner * rows, rows), rows)]

    def send_block(owner, peer):
        return [copies.make(block(buf, owner), block(buf, owner), copies.take(), peer) for buf in (kbuf, vbuf)]

    kv_x, kv_y = send_block(me, over_x), send_block(me, over_y)
    kv_d = send_block(over_x, over_y)
    kv_s = [send_block(owner, side) for owner in (me, over_x, over_y, over_d)]
    wo_first = copies.take(pieces)
    wo_side_first = copies.take(pieces)
    wo_pass_first = copies.take(pieces)
    y_first = copies.take(pieces)

    def columns(i):
        return pl.ds(pl.multiple_of(i * part, part), part)

    def send_wo(i):
        return copies.make(wo_hbm.at[:, columns(i)], wo.at[2, i], wo_first + i, over_y)

    def side_wo(i):
        return copies.make(wo_hbm.at[:, columns(i)], wo.at[1, i], wo_side_first + i, side)

    def pass_wo(i):
        return copies.make(wo.at[2, i], wo.at[3, i], wo_pass_first + i, side)

    def send_y(i):
        return copies.make(ysend.at[lax.rem(i, slots)], yrecv.at[i], y_first + i, over_x)

    def start(group):
        for copy in group:
            copy.start()

    def arrive(group):
        for copy in group:
            copy.wait_recv()

    send_x[0].start()
    send_a0.start()
    start(send_s)
    start(load_wq)

    def each(body):
        def step(i, _):
            body(i)
            return 0

        lax.fori_loop(0, pieces, step, 0)

    def load_wo(i):
        return pltpu.make_async_copy(wo_hbm.at[:, columns(i)], wo.at[0, i], local.at[8 + i])

    each(lambda i: load_wo(i).start())

    gain = gain_ref[...]

    def norm(row0, count, step=32):
        def body(i, _):
            at = pl.ds(pl.multiple_of(row0 + i * step, step), step)
            x = h[at, :].astype(F32)
            mean = jnp.sum(x, axis=1, keepdims=True) * (1.0 / width)
            x = x - mean
            var = jnp.sum(x * x, axis=1, keepdims=True) * (1.0 / width)
            h[at, :] = (x * lax.rsqrt(var + NORM_EPS) * gain).astype(BF16)
            return 0

        lax.fori_loop(0, count // step, body, 0)

    for i in range(2):
        load_x[i].wait()
    norm(0, rows)
    for copy in load_kv:
        copy.wait()

    def keys_values(i, _):
        at = pl.ds(pl.multiple_of(i * BLOCK, BLOCK), BLOCK)
        acc = None
        for j in range(4):
            dot = jnp.dot(
                h[at, j * quarter : (j + 1) * quarter], o[:, j * 2 * depth : (j + 1) * 2 * depth], preferred_element_type=F32
            )
            acc = dot if acc is None else acc + dot
        to = pl.ds(pl.multiple_of(me * rows + i * BLOCK, BLOCK), BLOCK)
        kbuf[to, :] = acc[:, :depth].astype(BF16)
        vbuf[to, :] = acc[:, depth:].astype(BF16)
        return 0

    lax.fori_loop(0, rows // BLOCK, keys_values, 0)
    start(kv_x)
    start(kv_y)
    start(kv_s[0])
    start(send_x[1:])

    def queries(head0, head_step, heads, row0, blocks):
        def body(t, _):
            head = head0 + head_step * lax.div(t, blocks)
            row = pl.multiple_of((row0 + lax.rem(t, blocks)) * BLOCK, BLOCK)
            col = pl.multiple_of(head * depth, depth)
            q = jnp.dot(h[pl.ds(row, BLOCK), :], wq[head], preferred_element_type=F32)
            o[pl.ds(row, BLOCK), pl.ds(col, depth)] = q.astype(BF16)
            return 0

        lax.fori_loop(0, heads * blocks, body, 0)

    factor = depth ** -0.5 * math.log2(math.e)

    def attention(head0, head_step, heads, row0, blocks):
        def body(t, _):
            head = head0 + head_step * lax.div(t, blocks)
            row = pl.multiple_of((row0 + lax.rem(t, blocks)) * BLOCK, BLOCK)
            col = pl.multiple_of(head * depth, depth)
            q = o[pl.ds(row, BLOCK), pl.ds(col, depth)]
            row_pos = pq_ref[pl.ds(row, BLOCK), :]

            def scores(j):
                lo = j * KEYS
                dot = lax.dot_general(q, kbuf[lo : lo + KEYS, :], (((1,), (1,)), ((), ())), preferred_element_type=F32)
                dot = jnp.where(pk_ref[:, lo : lo + KEYS] <= row_pos, dot, NEG)
                s[j % 2] = dot
                return jnp.max(dot, axis=1, keepdims=True)

            steps = keys // KEYS
            top = scores(0)
            best = total = acc = None
            for j in range(steps):
                after = scores(j + 1) if j + 1 < steps else None
                new = jnp.maximum(best, top) if j else top
                p = jnp.exp2((s[j % 2] - new) * factor)
                sums = jnp.sum(p, axis=1, keepdims=True)
                pv = jnp.dot(p.astype(BF16), vbuf[j * KEYS : (j + 1) * KEYS, :], preferred_element_type=F32)
                if j:
                    scale = jnp.exp2((best - new) * factor)
                    total = total * scale + sums
                    acc = acc * scale + pv
                else:
                    total, acc = sums, pv
                best, top = new, after
            o[pl.ds(row, BLOCK), pl.ds(col, depth)] = (acc * (1.0 / total)).astype(BF16)
            return 0

        lax.fori_loop(0, heads * blocks, body, 0)

    for copy in load_wq:
        copy.wait()
    queries(0, 1, 2, 0, 2)
    arrive(kv_x)
    start(kv_d)
    start(kv_s[1])
    start([send_a1, send_b])
    each(lambda i: send_wo(i).start())
    arrive(send_s)
    queries(2, 1, 2, 0, 2)
    arrive(kv_y)
    start(kv_s[2])
    arrive(kv_d)
    start(kv_s[3])
    each(lambda i: side_wo(i).start())
    for group in kv_s:
        arrive(group)
    keep = [pltpu.make_async_copy(kbuf, k_hbm, out_sem.at[2]), pltpu.make_async_copy(vbuf, v_hbm, out_sem.at[3])]
    start(keep)

    attention(0, 1, 4, 0, 2)
    arrive(send_x[:2])
    norm(rows, BLOCK)
    queries(0, 1, 4, 2, 1)
    attention(0, 1, 4, 2, 1)
    arrive([send_a0, send_a1])
    pass_a.start()
    queries(4, 1, 1, 0, 3)
    pass_a.wait_recv()
    queries(6, 1, 1, 0, 3)
    attention(4, 2, 2, 0, 3)
    arrive(send_x[2:])
    norm(rows + BLOCK, BLOCK)
    queries(0, 1, 4, 3, 1)
    queries(4, 2, 2, 3, 1)
    attention(0, 1, 4, 3, 1)
    attention(4, 2, 2, 3, 1)
    send_b.wait_recv()
    pass_b.start()
    queries(5, 1, 1, 2, 2)
    attention(5, 1, 1, 2, 2)
    pass_b.wait_recv()
    queries(7, 1, 1, 2, 2)
    attention(7, 1, 1, 2, 2)

    def weights_ready(i):
        send_wo(i).wait_recv()
        pass_wo(i).start()
        load_wo(i).wait()
        side_wo(i).wait_recv()
        pass_wo(i).wait_recv()

    def product(row0, i):
        acc = None
        for b in range(4):
            dot = jnp.dot(o[row0 : row0 + rows, b * 2 * depth : (b + 1) * 2 * depth], wo[b, i], preferred_element_type=F32)
            acc = dot if acc is None else acc + dot
        return acc

    def share(i):
        weights_ready(i)
        ysend[lax.rem(i, slots)] = product(rows, i).astype(BF16)
        send_y(i).start()

    def finish(i):
        value = product(0, i)
        send_y(i).wait_recv()
        yout[lax.rem(i, 2)] = (value + yrecv[i].astype(F32)).astype(BF16)
        store_y(i).start()

    def store_y(i):
        return pltpu.make_async_copy(yout.at[lax.rem(i, 2)], y_hbm.at[:, columns(i)], out_sem.at[lax.rem(i, 2)])

    share(0)
    queries(5, 2, 2, 0, 2)
    attention(5, 2, 2, 0, 2)

    def step(i, _):
        @pl.when(i >= slots)
        def _():
            send_y(i - slots).wait_send()

        share(i)

        @pl.when(i >= 3)
        def _():
            store_y(i - 3).wait()

        finish(i - 1)
        return 0

    lax.fori_loop(1, pieces, step, 0)
    store_y(pieces - 3).wait()
    finish(pieces - 1)

    for copy in send_x + [send_a0, send_a1, send_b, pass_a, pass_b] + send_s + kv_x + kv_y + kv_d + sum(kv_s, []):
        copy.wait_send()
    def sent(i):
        send_wo(i).wait_send()
        side_wo(i).wait_send()
        pass_wo(i).wait_send()

        @pl.when(i >= pieces - slots)
        def _():
            send_y(i).wait_send()

    each(sent)
    for copy in keep:
        copy.wait()
    store_y(pieces - 2).wait()
    store_y(pieces - 1).wait()


def solution(mesh):
    def local_step(x_loc, ln_gain, wq_loc, w_kv, wo_loc, positions):
        me = lax.axis_index("model")
        rows, width = x_loc.shape
        keys = positions.shape[0]
        depth = w_kv.shape[1] // 2
        pieces = 8
        part = width // pieces

        def positions_of(device):
            return lax.dynamic_slice(positions, (device * rows,), (rows,))

        row_pos = jnp.concatenate([positions_of(me), positions_of(me ^ 2)])
        row_pos = row_pos.reshape(2 * rows, 1)
        whole = pl.BlockSpec(memory_space=pl.ANY)
        vmem = pl.BlockSpec(memory_space=pltpu.VMEM)
        heads = 8
        return pl.pallas_call(
            kernel,
            out_shape=[
                jax.ShapeDtypeStruct((rows, width), BF16),
                jax.ShapeDtypeStruct((keys, depth), BF16),
                jax.ShapeDtypeStruct((keys, depth), BF16),
            ],
            in_specs=[whole] * 4 + [vmem] * 3,
            out_specs=[whole] * 3,
            scratch_shapes=[
                pltpu.VMEM((2 * rows, width), BF16),
                pltpu.VMEM((keys, depth), BF16),
                pltpu.VMEM((keys, depth), BF16),
                pltpu.VMEM((heads, width, depth), BF16),
                pltpu.VMEM((4, pieces, 2 * depth, part), BF16),
                pltpu.VMEM((2 * rows, heads * depth), BF16),
                pltpu.VMEM((2, BLOCK, KEYS), F32),
                pltpu.VMEM((4, rows, part), BF16),
                pltpu.VMEM((pieces, rows, part), BF16),
                pltpu.VMEM((2, rows, part), BF16),
                pltpu.SemaphoreType.DMA((N_COPIES,)),
                pltpu.SemaphoreType.DMA((N_COPIES,)),
                pltpu.SemaphoreType.DMA((16,)),
                pltpu.SemaphoreType.DMA((4,)),
            ],
            compiler_params=pltpu.CompilerParams(collective_id=0, has_side_effects=True, vmem_limit_bytes=VMEM_LIMIT),
            name="layer",
        )(x_loc, wq_loc, w_kv, wo_loc, ln_gain.reshape(1, width), row_pos, positions.reshape(1, keys))

    return jax.shard_map(
        local_step,
        mesh=mesh,
        in_specs=(P("model", None), P(None), P(None, "model"), P(None, None), P("model", None), P(None)),
        out_specs=(P("model", None), P(None, None), P(None, None)),
        check_vma=False,
    )
```

```python
import functools
import math

import jax
import jax.numpy as jnp
from jax import lax
from jax.experimental import pallas as pl
from jax.experimental.pallas import tpu as pltpu
from jax.sharding import PartitionSpec as P

NORM_EPS = 1e-6
NEG = -1e30
F32 = jnp.float32
BF16 = jnp.bfloat16
MESH = pl.DeviceIdType.MESH
VMEM_LIMIT = 67_000_000

BLOCK = 256
ROWS = 128
KEYS = 1024
X_CUT = (0, 64, 256, 384, 512)
A_CUT = 1024
B_CUT = 3072
FIRST = 384


class Copies:
    def __init__(self, send, recv):
        self.send, self.recv, self.used = send, recv, 0

    def take(self, n=1):
        first = self.used
        self.used += n
        return first

    def make(self, src, dst, i, peer):
        return pltpu.make_async_remote_copy(
            src_ref=src, dst_ref=dst, send_sem=self.send.at[i], recv_sem=self.recv.at[i], device_id=(peer,), device_id_type=MESH
        )


N_COPIES = 67


def kernel(
    x_hbm, wq_hbm, wkv_hbm, wo_hbm, gain_ref, pq_ref, pk_ref,
    y_hbm, k_hbm, v_hbm,
    h, kbuf, vbuf, wq, wo, o, s, ysend, yrecv, yout,
    send, recv, local, out_sem,
):
    me = lax.axis_index("model")
    rows = x_hbm.shape[0]
    width = x_hbm.shape[1]
    depth = kbuf.shape[1]
    keys = kbuf.shape[0]
    pieces = wo.shape[1]
    part = width // pieces
    slots = ysend.shape[0]

    def flip(bit):
        return me + bit - 2 * bit * lax.rem(lax.div(me, bit), 2)

    side, over_x, over_y = flip(1), flip(2), flip(4)
    over_d = over_x + over_y - me
    copies = Copies(send, recv)

    half = rows // 2
    load_x = [pltpu.make_async_copy(x_hbm.at[i * half : (i + 1) * half], h.at[i * half : (i + 1) * half], local.at[i]) for i in range(2)]
    quarter = width // 4
    load_kv = [
        pltpu.make_async_copy(wkv_hbm.at[j * quarter : (j + 1) * quarter], o.at[:, j * 2 * depth : (j + 1) * 2 * depth], local.at[2 + j])
        for j in range(4)
    ]
    load_wq = [pltpu.make_async_copy(wq_hbm.at[:, i * depth : (i + 1) * depth], wq.at[i], local.at[6 + i]) for i in range(2)]
    for copy in load_x + load_kv:
        copy.start()

    barrier = pltpu.get_barrier_semaphore()
    for peer in (side, over_x, over_y):
        pl.semaphore_signal(barrier, inc=1, device_id=(peer,), device_id_type=MESH)
    pl.semaphore_wait(barrier, 3)

    send_x = []
    for a, b in zip(X_CUT, X_CUT[1:]):
        send_x.append(copies.make(x_hbm.at[a:b], h.at[rows + a : rows + b], copies.take(), over_x))
    send_a0 = copies.make(wq_hbm.at[0:A_CUT, 0:depth], wq.at[4, 0:A_CUT], copies.take(), over_y)
    send_a1 = copies.make(wq_hbm.at[A_CUT:width, 0:depth], wq.at[4, A_CUT:width], copies.take(), over_y)
    b_cuts = ((0, B_CUT), (B_CUT, width))
    send_b = [copies.make(wq_hbm.at[a:b, depth : 2 * depth], wq.at[5, a:b], copies.take(), over_y) for a, b in b_cuts]
    send_s = [copies.make(wq_hbm.at[:, i * depth : (i + 1) * depth], wq.at[2 + i], copies.take(), side) for i in range(2)]
    pass_a = copies.make(wq.at[4], wq.at[6], copies.take(), side)
    pass_b = [copies.make(wq.at[5, a:b], wq.at[7, a:b], copies.take(), side) for a, b in b_cuts]

    def block(buf, owner):
        return buf.at[pl.ds(pl.multiple_of(owner * rows, rows), rows)]

    def send_block(owner, peer):
        return [copies.make(block(buf, owner), block(buf, owner), copies.take(), peer) for buf in (kbuf, vbuf)]

    kv_x, kv_y = send_block(me, over_x), send_block(me, over_y)
    k_d = copies.make(block(kbuf, over_x), block(kbuf, over_x), copies.take(), over_y)
    v_d = copies.make(block(vbuf, over_y), block(vbuf, over_y), copies.take(), over_x)
    kv_s = [send_block(owner, side) for owner in (me, over_x, over_y, over_d)]
    wo_first = copies.take(pieces)
    wo_side_first = copies.take(pieces)
    wo_pass_first = copies.take(pieces)
    y_first = copies.take(pieces)
    last = pieces - 1
    cut = part // 2
    y_early = copies.take(2)
    wo_last, wo_pass_last, y_last = copies.take(2), copies.take(2), copies.take(2)

    def columns(i):
        return pl.ds(pl.multiple_of(i * part, part), part)

    def send_wo(i):
        return copies.make(wo_hbm.at[:, columns(i)], wo.at[2, i], wo_first + i, over_y)

    def side_wo(i):
        return copies.make(wo_hbm.at[:, columns(i)], wo.at[1, i], wo_side_first + i, side)

    def pass_wo(i):
        return copies.make(wo.at[2, i], wo.at[3, i], wo_pass_first + i, side)

    def send_wo_last(n):
        src = wo_hbm.at[:, last * part + n * cut : last * part + (n + 1) * cut]
        return copies.make(src, wo.at[2, last, :, n * cut : (n + 1) * cut], wo_last + n, over_y)

    def pass_wo_last(n):
        at = slice(n * cut, (n + 1) * cut)
        return copies.make(wo.at[2, last, :, at], wo.at[3, last, :, at], wo_pass_last + n, side)

    def send_y_last(n):
        at = slice(n * cut, (n + 1) * cut)
        return copies.make(ysend.at[last % slots, :, at], yrecv.at[last, :, at], y_last + n, over_x)

    def send_y_first(n):
        at = slice(0, FIRST) if n == 0 else slice(FIRST, rows)
        return copies.make(ysend.at[0, at], yrecv.at[0, at], y_early + n, over_x)

    def send_y(i):
        return copies.make(ysend.at[lax.rem(i, slots)], yrecv.at[i], y_first + i, over_x)

    def start(group):
        for copy in group:
            copy.start()

    def arrive(group):
        for copy in group:
            copy.wait_recv()

    assert copies.used == N_COPIES

    send_x[0].start()
    send_a0.start()
    start(send_s)
    start(load_wq)

    def load_wo(i):
        return pltpu.make_async_copy(wo_hbm.at[:, columns(i)], wo.at[0, i], local.at[8 + i])

    gain = gain_ref[...]

    def norm(row0, count, step=32):
        def body(i, _):
            at = pl.ds(pl.multiple_of(row0 + i * step, step), step)
            x = h[at, :].astype(F32)
            mean = jnp.sum(x, axis=1, keepdims=True) * (1.0 / width)
            x = x - mean
            var = jnp.sum(x * x, axis=1, keepdims=True) * (1.0 / width)
            h[at, :] = (x * lax.rsqrt(var + NORM_EPS) * gain).astype(BF16)
            return 0

        lax.fori_loop(0, count // step, body, 0)

    for i in range(2):
        load_x[i].wait()
    norm(0, rows)
    for copy in load_kv:
        copy.wait()

    def keys_values(i, _):
        at = pl.ds(pl.multiple_of(i * BLOCK, BLOCK), BLOCK)
        acc = None
        for j in range(4):
            dot = jnp.dot(
                h[at, j * quarter : (j + 1) * quarter], o[:, j * 2 * depth : (j + 1) * 2 * depth], preferred_element_type=F32
            )
            acc = dot if acc is None else acc + dot
        to = pl.ds(pl.multiple_of(me * rows + i * BLOCK, BLOCK), BLOCK)
        kbuf[to, :] = acc[:, :depth].astype(BF16)
        vbuf[to, :] = acc[:, depth:].astype(BF16)
        return 0

    lax.fori_loop(0, rows // BLOCK, keys_values, 0)
    start(kv_x)
    start(kv_y)
    start(kv_s[0])

    def queries(head0, heads, block0, blocks, step=BLOCK, skip=8):
        def body(t, _):
            head = head0 + lax.div(t, blocks)
            head = head + lax.div(head, skip)
            row = pl.multiple_of((block0 + lax.rem(t, blocks)) * step, step)
            col = pl.multiple_of(head * depth, depth)
            q = jnp.dot(h[pl.ds(row, step), :], wq[head], preferred_element_type=F32)
            o[pl.ds(row, step), pl.ds(col, depth)] = q.astype(BF16)
            return 0

        lax.fori_loop(0, heads * blocks, body, 0)

    factor = depth ** -0.5 * math.log2(math.e)

    def attention(pair0, pairs, block0, blocks):
        def body(t, _):
            pair = pair0 + lax.div(t, blocks)
            head = 2 * pair - lax.div(pair, 3)
            other = head + 1 + lax.div(pair, 2)
            at = pl.ds(pl.multiple_of((block0 + lax.rem(t, blocks)) * ROWS, ROWS), ROWS)
            one = pl.ds(pl.multiple_of(head * depth, depth), depth)
            two = pl.ds(pl.multiple_of(other * depth, depth), depth)
            q = jnp.concatenate([o[at, one], o[at, two]], axis=0)
            row_pos = pq_ref[at, :]
            row_pos = jnp.concatenate([row_pos, row_pos], axis=0)

            def scores(j):
                lo = j * KEYS
                dot = lax.dot_general(q, kbuf[lo : lo + KEYS, :], (((1,), (1,)), ((), ())), preferred_element_type=F32)
                dot = jnp.where(pk_ref[:, lo : lo + KEYS] <= row_pos, dot, NEG)
                s[j % 2] = dot
                return jnp.max(dot, axis=1, keepdims=True)

            steps = keys // KEYS
            top = scores(0)
            best = total = acc = None
            for j in range(steps):
                after = scores(j + 1) if j + 1 < steps else None
                new = jnp.maximum(best, top) if j else top
                p = jnp.exp2((s[j % 2] - new) * factor)
                sums = jnp.sum(p, axis=1, keepdims=True)
                pv = jnp.dot(p.astype(BF16), vbuf[j * KEYS : (j + 1) * KEYS, :], preferred_element_type=F32)
                if j:
                    scale = jnp.exp2((best - new) * factor)
                    total = total * scale + sums
                    acc = acc * scale + pv
                else:
                    total, acc = sums, pv
                best, top = new, after
            acc = (acc * (1.0 / total)).astype(BF16)
            o[at, one] = acc[:ROWS]
            o[at, two] = acc[ROWS:]
            return 0

        lax.fori_loop(0, pairs * blocks, body, 0)

    def each(body, first=0, end=None):
        def step(i, _):
            body(i)
            return 0

        lax.fori_loop(first, pieces if end is None else end, step, 0)

    for copy in load_wq:
        copy.wait()
    queries(0, 2, 0, 2)
    arrive(kv_x)
    k_d.start()
    start(kv_s[1])
    arrive(kv_y)
    v_d.start()
    start(kv_s[2])
    start([send_a1] + send_b)
    start(send_x[1:])
    each(lambda i: send_wo(i).start(), 0, last)
    start([send_wo_last(0), send_wo_last(1)])
    arrive(send_s)
    queries(2, 2, 0, 2)
    arrive([k_d, v_d])
    start(kv_s[3])
    each(lambda i: side_wo(i).start())
    each(lambda i: load_wo(i).start())
    for group in kv_s:
        arrive(group)
    keep = [pltpu.make_async_copy(kbuf, k_hbm, out_sem.at[2]), pltpu.make_async_copy(vbuf, v_hbm, out_sem.at[3])]
    start(keep)

    attention(0, 2, 0, 4)
    arrive([send_a0, send_a1])
    pass_a.start()
    queries(4, 1, 0, 2)
    pass_a.wait_recv()
    queries(6, 1, 0, 2)
    attention(2, 1, 0, 4)
    arrive(send_x[:2])
    norm(rows, 256)
    queries(0, 6, 2, 1, skip=5)
    attention(0, 3, 4, 2)
    send_x[2].wait_recv()
    norm(rows + 256, 128)
    queries(0, 6, 6, 1, step=ROWS, skip=5)
    attention(0, 3, 6, 1)
    send_b[0].wait_recv()
    pass_b[0].start()
    send_b[1].wait_recv()
    pass_b[1].start()
    queries(5, 1, 4, 3, step=ROWS)
    arrive(pass_b)
    queries(7, 1, 4, 3, step=ROWS)
    attention(3, 1, 4, 3)

    def product(row0, count, i, cols=slice(None)):
        acc = None
        for b in range(4):
            dot = jnp.dot(
                o[row0 : row0 + count, b * 2 * depth : (b + 1) * 2 * depth], wo[b, i, :, cols], preferred_element_type=F32
            )
            acc = dot if acc is None else acc + dot
        return acc

    def weights_ready(i):
        send_wo(i).wait_recv()
        pass_wo(i).start()
        load_wo(i).wait()
        side_wo(i).wait_recv()
        pass_wo(i).wait_recv()

    def share(i):
        weights_ready(i)
        ysend[lax.rem(i, slots)] = product(rows, rows, i).astype(BF16)
        send_y(i).start()

    def finish(i):
        value = product(0, rows, i)
        send_y(i).wait_recv()
        yout[lax.rem(i, 2)] = (value + yrecv[i].astype(F32)).astype(BF16)
        store_y(i).start()

    def store_y(i):
        return pltpu.make_async_copy(yout.at[lax.rem(i, 2)], y_hbm.at[:, columns(i)], out_sem.at[lax.rem(i, 2)])

    weights_ready(0)
    ysend[0, 0:FIRST] = product(rows, FIRST, 0).astype(BF16)
    send_y_first(0).start()
    send_x[3].wait_recv()
    norm(rows + FIRST, rows - FIRST)
    queries(0, 8, 7, 1, step=ROWS)
    attention(0, 4, 7, 1)
    ysend[0, FIRST:rows] = product(rows + FIRST, rows - FIRST, 0).astype(BF16)
    send_y_first(1).start()
    share(1)
    queries(5, 1, 0, 2)
    queries(7, 1, 0, 2)
    attention(3, 1, 0, 4)
    share(2)
    value = product(0, rows, 0)
    send_y_first(0).wait_recv()
    send_y_first(1).wait_recv()
    yout[0] = (value + yrecv[0].astype(F32)).astype(BF16)
    store_y(0).start()
    finish(1)

    def step(i, _):
        @pl.when(i == slots)
        def _():
            send_y_first(0).wait_send()
            send_y_first(1).wait_send()

        @pl.when(i > slots)
        def _():
            send_y(i - slots).wait_send()

        share(i)
        store_y(i - 3).wait()
        finish(i - 1)
        return 0

    lax.fori_loop(3, last, step, 0)
    send_y(last - slots).wait_send()
    load_wo(last).wait()
    side_wo(last).wait_recv()
    for n in range(2):
        at = slice(n * cut, (n + 1) * cut)
        send_wo_last(n).wait_recv()
        pass_wo_last(n).start()
        pass_wo_last(n).wait_recv()
        ysend[last % slots, :, at] = product(rows, rows, last, at).astype(BF16)
        send_y_last(n).start()
        if n == 0:
            store_y(last - 3).wait()
            finish(last - 1)
    store_y(last - 2).wait()
    for n in range(2):
        at = slice(n * cut, (n + 1) * cut)
        value = product(0, rows, last, at)
        send_y_last(n).wait_recv()
        yout[last % 2, :, at] = (value + yrecv[last, :, at].astype(F32)).astype(BF16)
    store_y(last).start()

    for copy in send_x + [send_a0, send_a1, pass_a, k_d, v_d] + send_b + pass_b + send_s + kv_x + kv_y + sum(kv_s, []):
        copy.wait_send()

    def sent(i):
        send_wo(i).wait_send()
        side_wo(i).wait_send()
        pass_wo(i).wait_send()

        @pl.when(i > last - slots)
        def _():
            send_y(i).wait_send()

    each(sent, 0, last)
    side_wo(last).wait_send()
    for n in range(2):
        send_wo_last(n).wait_send()
        pass_wo_last(n).wait_send()
        send_y_last(n).wait_send()
    for copy in keep:
        copy.wait()
    store_y(last - 1).wait()
    store_y(last).wait()


def solution(mesh):
    def local_step(x_loc, ln_gain, wq_loc, w_kv, wo_loc, positions):
        me = lax.axis_index("model")
        rows, width = x_loc.shape
        keys = positions.shape[0]
        depth = w_kv.shape[1] // 2
        pieces = 8
        part = width // pieces

        def positions_of(device):
            return lax.dynamic_slice(positions, (device * rows,), (rows,))

        row_pos = jnp.concatenate([positions_of(me), positions_of(me ^ 2)])
        row_pos = row_pos.reshape(2 * rows, 1)
        whole = pl.BlockSpec(memory_space=pl.ANY)
        vmem = pl.BlockSpec(memory_space=pltpu.VMEM)
        heads = 8
        return pl.pallas_call(
            kernel,
            out_shape=[
                jax.ShapeDtypeStruct((rows, width), BF16),
                jax.ShapeDtypeStruct((keys, depth), BF16),
                jax.ShapeDtypeStruct((keys, depth), BF16),
            ],
            in_specs=[whole] * 4 + [vmem] * 3,
            out_specs=[whole] * 3,
            scratch_shapes=[
                pltpu.VMEM((2 * rows, width), BF16),
                pltpu.VMEM((keys, depth), BF16),
                pltpu.VMEM((keys, depth), BF16),
                pltpu.VMEM((heads, width, depth), BF16),
                pltpu.VMEM((4, pieces, 2 * depth, part), BF16),
                pltpu.VMEM((2 * rows, heads * depth), BF16),
                pltpu.VMEM((2, BLOCK, KEYS), F32),
                pltpu.VMEM((4, rows, part), BF16),
                pltpu.VMEM((pieces, rows, part), BF16),
                pltpu.VMEM((2, rows, part), BF16),
                pltpu.SemaphoreType.DMA((N_COPIES,)),
                pltpu.SemaphoreType.DMA((N_COPIES,)),
                pltpu.SemaphoreType.DMA((16,)),
                pltpu.SemaphoreType.DMA((4,)),
            ],
            compiler_params=pltpu.CompilerParams(collective_id=0, has_side_effects=True, vmem_limit_bytes=VMEM_LIMIT),
            name="layer",
        )(x_loc, wq_loc, w_kv, wo_loc, ln_gain.reshape(1, width), row_pos, positions.reshape(1, keys))

    return jax.shard_map(
        local_step,
        mesh=mesh,
        in_specs=(P("model", None), P(None), P(None, "model"), P(None, None), P("model", None), P(None)),
        out_specs=(P("model", None), P(None, None), P(None, None)),
        check_vma=False,
    )
```

```python
import functools
import math

import jax
import jax.numpy as jnp
from jax import lax
from jax.experimental import pallas as pl
from jax.experimental.pallas import tpu as pltpu
from jax.sharding import PartitionSpec as P

NORM_EPS = 1e-6
NEG = -1e30
F32 = jnp.float32
BF16 = jnp.bfloat16
MESH = pl.DeviceIdType.MESH
VMEM_LIMIT = 67_000_000

BLOCK = 256
ROWS = 128
KEYS = 1024
X_CUT = (0, 64, 256, 384, 512)
A_CUT = 1024
B_CUT = 3072
FIRST = 384
EARLY = 3


class Copies:
    def __init__(self, send, recv):
        self.send, self.recv, self.used = send, recv, 0

    def take(self, n=1):
        first = self.used
        self.used += n
        return first

    def make(self, src, dst, i, peer):
        return pltpu.make_async_remote_copy(
            src_ref=src, dst_ref=dst, send_sem=self.send.at[i], recv_sem=self.recv.at[i], device_id=(peer,), device_id_type=MESH
        )


N_COPIES = 97


def kernel(
    x_hbm, wq_hbm, wkv_hbm, wo_hbm, gain_ref, pos_ref, pk_ref,
    y_hbm, k_hbm, v_hbm,
    h, kbuf, vbuf, wq, wo, o, s, ysend, yrecv, yout, pq_ref,
    send, recv, local, out_sem,
):
    me = lax.axis_index("model")
    rows = x_hbm.shape[0]
    width = x_hbm.shape[1]
    depth = kbuf.shape[1]
    keys = kbuf.shape[0]
    pieces = wo.shape[1]
    part = width // pieces
    slots = ysend.shape[0]

    def flip(bit):
        return me + bit - 2 * bit * lax.rem(lax.div(me, bit), 2)

    side, over_x, over_y = flip(1), flip(2), flip(4)
    over_d = over_x + over_y - me
    copies = Copies(send, recv)

    half = rows // 2
    load_x = [pltpu.make_async_copy(x_hbm.at[i * half : (i + 1) * half], h.at[i * half : (i + 1) * half], local.at[i]) for i in range(2)]
    quarter = width // 4
    load_kv = [
        pltpu.make_async_copy(wkv_hbm.at[j * quarter : (j + 1) * quarter], o.at[:, j * 2 * depth : (j + 1) * 2 * depth], local.at[2 + j])
        for j in range(4)
    ]
    load_wq = [pltpu.make_async_copy(wq_hbm.at[:, i * depth : (i + 1) * depth], wq.at[i], local.at[6 + i]) for i in range(2)]
    for copy in load_x + load_kv:
        copy.start()

    barrier = pltpu.get_barrier_semaphore()
    for peer in (side, over_x, over_y):
        pl.semaphore_signal(barrier, inc=1, device_id=(peer,), device_id_type=MESH)
    pl.semaphore_wait(barrier, 3)

    send_x = []
    for a, b in zip(X_CUT, X_CUT[1:]):
        send_x.append(copies.make(x_hbm.at[a:b], h.at[rows + a : rows + b], copies.take(), over_x))
    send_a0 = copies.make(wq_hbm.at[0:A_CUT, 0:depth], wq.at[4, 0:A_CUT], copies.take(), over_y)
    send_a1 = copies.make(wq_hbm.at[A_CUT:width, 0:depth], wq.at[4, A_CUT:width], copies.take(), over_y)
    b_cuts = ((0, B_CUT), (B_CUT, width))
    send_b = [copies.make(wq_hbm.at[a:b, depth : 2 * depth], wq.at[5, a:b], copies.take(), over_y) for a, b in b_cuts]
    send_s = [copies.make(wq_hbm.at[:, i * depth : (i + 1) * depth], wq.at[2 + i], copies.take(), side) for i in range(2)]
    pass_a = copies.make(wq.at[4], wq.at[6], copies.take(), side)
    pass_b = [copies.make(wq.at[5, a:b], wq.at[7, a:b], copies.take(), side) for a, b in b_cuts]

    def block(buf, owner):
        return buf.at[pl.ds(pl.multiple_of(owner * rows, rows), rows)]

    def send_block(owner, peer):
        return [copies.make(block(buf, owner), block(buf, owner), copies.take(), peer) for buf in (kbuf, vbuf)]

    kv_x, kv_y = send_block(me, over_x), send_block(me, over_y)
    kv_d = send_block(over_y, over_x)
    kv_s = [send_block(owner, side) for owner in (me, over_x, over_y, over_d)]
    wo_first = copies.take(pieces)
    wo_side_first = copies.take(pieces)
    wo_pass_first = copies.take(pieces)
    y_first = copies.take(pieces)
    y_early = copies.take(2 * EARLY)

    def columns(i):
        return pl.ds(pl.multiple_of(i * part, part), part)

    def send_wo(i):
        return copies.make(wo_hbm.at[:, columns(i)], wo.at[2, i], wo_first + i, over_y)

    def side_wo(i):
        return copies.make(wo_hbm.at[:, columns(i)], wo.at[1, i], wo_side_first + i, side)

    def pass_wo(i):
        return copies.make(wo.at[2, i], wo.at[3, i], wo_pass_first + i, side)

    def send_early(i, n):
        at = slice(0, FIRST) if n == 0 else slice(FIRST, rows)
        return copies.make(ysend.at[i, at], yrecv.at[i, at], y_early + 2 * i + n, over_x)

    def send_y(i):
        return copies.make(ysend.at[lax.rem(i, slots)], yrecv.at[i], y_first + i, over_x)

    def start(group):
        for copy in group:
            copy.start()

    def arrive(group):
        for copy in group:
            copy.wait_recv()

    assert copies.used == N_COPIES

    send_x[0].start()
    send_a0.start()
    start(send_s)
    start(load_wq)

    def load_wo(i):
        return pltpu.make_async_copy(wo_hbm.at[:, columns(i)], wo.at[0, i], local.at[8 + i])

    gain = gain_ref[...]

    def norm(row0, count, step=32):
        def body(i, _):
            at = pl.ds(pl.multiple_of(row0 + i * step, step), step)
            x = h[at, :].astype(F32)
            mean = jnp.sum(x, axis=1, keepdims=True) * (1.0 / width)
            x = x - mean
            var = jnp.sum(x * x, axis=1, keepdims=True) * (1.0 / width)
            h[at, :] = (x * lax.rsqrt(var + NORM_EPS) * gain).astype(BF16)
            return 0

        lax.fori_loop(0, count // step, body, 0)

    for i in range(2):
        load_x[i].wait()
    norm(0, rows)
    for copy in load_kv:
        copy.wait()

    def keys_values(i, _):
        at = pl.ds(pl.multiple_of(i * BLOCK, BLOCK), BLOCK)
        acc = None
        for j in range(4):
            dot = jnp.dot(
                h[at, j * quarter : (j + 1) * quarter], o[:, j * 2 * depth : (j + 1) * 2 * depth], preferred_element_type=F32
            )
            acc = dot if acc is None else acc + dot
        to = pl.ds(pl.multiple_of(me * rows + i * BLOCK, BLOCK), BLOCK)
        kbuf[to, :] = acc[:, :depth].astype(BF16)
        vbuf[to, :] = acc[:, depth:].astype(BF16)
        return 0

    lax.fori_loop(0, rows // BLOCK, keys_values, 0)
    start(kv_x)
    start(kv_y)
    start(kv_s[0])

    def queries(head0, heads, block0, blocks, step=BLOCK, skip=8):
        def body(t, _):
            head = head0 + lax.div(t, blocks)
            head = head + lax.div(head, skip)
            row = pl.multiple_of((block0 + lax.rem(t, blocks)) * step, step)
            col = pl.multiple_of(head * depth, depth)
            q = jnp.dot(h[pl.ds(row, step), :], wq[head], preferred_element_type=F32)
            o[pl.ds(row, step), pl.ds(col, depth)] = q.astype(BF16)
            return 0

        lax.fori_loop(0, heads * blocks, body, 0)

    factor = depth ** -0.5 * math.log2(math.e)

    def attention(pair0, pairs, block0, blocks):
        def body(t, _):
            pair = pair0 + lax.div(t, blocks)
            head = 2 * pair - lax.div(pair, 3)
            other = head + 1 + lax.div(pair, 2)
            at = pl.ds(pl.multiple_of((block0 + lax.rem(t, blocks)) * ROWS, ROWS), ROWS)
            one = pl.ds(pl.multiple_of(head * depth, depth), depth)
            two = pl.ds(pl.multiple_of(other * depth, depth), depth)
            q = jnp.concatenate([o[at, one], o[at, two]], axis=0)
            row_pos = pq_ref[at, 0:1]
            row_pos = jnp.concatenate([row_pos, row_pos], axis=0)

            def scores(j):
                lo = j * KEYS
                dot = lax.dot_general(q, kbuf[lo : lo + KEYS, :], (((1,), (1,)), ((), ())), preferred_element_type=F32)
                dot = jnp.where(pk_ref[:, lo : lo + KEYS] <= row_pos, dot, NEG)
                s[j % 2] = dot
                return jnp.max(dot, axis=1, keepdims=True)

            steps = keys // KEYS
            top = scores(0)
            best = total = acc = None
            for j in range(steps):
                after = scores(j + 1) if j + 1 < steps else None
                new = jnp.maximum(best, top) if j else top
                p = jnp.exp2((s[j % 2] - new) * factor)
                sums = jnp.sum(p, axis=1, keepdims=True)
                pv = jnp.dot(p.astype(BF16), vbuf[j * KEYS : (j + 1) * KEYS, :], preferred_element_type=F32)
                if j:
                    scale = jnp.exp2((best - new) * factor)
                    total = total * scale + sums
                    acc = acc * scale + pv
                else:
                    total, acc = sums, pv
                best, top = new, after
            acc = (acc * (1.0 / total)).astype(BF16)
            o[at, one] = acc[:ROWS]
            o[at, two] = acc[ROWS:]
            return 0

        lax.fori_loop(0, pairs * blocks, body, 0)

    lanes = pq_ref.shape[1]
    for n, device in enumerate((me, over_x)):
        for b in range(rows // lanes):
            line = pos_ref[pl.ds(device * (rows // lanes) + b, 1), :]
            first = n * rows + b * lanes
            pq_ref[first : first + lanes, :] = jnp.broadcast_to(line, (lanes, lanes)).T

    def each(body, first=0, end=None):
        def step(i, _):
            body(i)
            return 0

        lax.fori_loop(first, pieces if end is None else end, step, 0)

    for copy in load_wq:
        copy.wait()
    queries(0, 2, 0, 2)
    start([send_a1] + send_b)
    each(lambda i: send_wo(i).start())
    arrive(kv_y)
    start(kv_d)
    start(send_x[1:])
    start(kv_s[2])
    arrive(kv_x)
    start(kv_s[1])
    arrive(send_s)
    queries(2, 2, 0, 2)
    arrive(kv_d)
    start(kv_s[3])
    each(lambda i: side_wo(i).start())
    each(lambda i: load_wo(i).start())
    for group in kv_s:
        arrive(group)
    keep = [pltpu.make_async_copy(kbuf, k_hbm, out_sem.at[2]), pltpu.make_async_copy(vbuf, v_hbm, out_sem.at[3])]
    start(keep)

    attention(0, 2, 0, 4)
    arrive([send_a0, send_a1])
    pass_a.start()
    queries(4, 1, 0, 2)
    pass_a.wait_recv()
    queries(6, 1, 0, 2)
    attention(2, 1, 0, 4)
    arrive(send_x[:2])
    norm(rows, 256)
    queries(0, 6, 2, 1, skip=5)
    attention(0, 3, 4, 2)
    send_x[2].wait_recv()
    norm(rows + 256, 128)
    queries(0, 6, 6, 1, step=ROWS, skip=5)
    attention(0, 3, 6, 1)
    send_b[0].wait_recv()
    pass_b[0].start()
    send_b[1].wait_recv()
    pass_b[1].start()
    queries(5, 1, 4, 3, step=ROWS)
    arrive(pass_b)
    queries(7, 1, 4, 3, step=ROWS)
    attention(3, 1, 4, 3)

    def product(row0, count, i):
        acc = None
        for b in range(4):
            dot = jnp.dot(o[row0 : row0 + count, b * 2 * depth : (b + 1) * 2 * depth], wo[b, i], preferred_element_type=F32)
            acc = dot if acc is None else acc + dot
        return acc

    def weights_ready(i):
        send_wo(i).wait_recv()
        pass_wo(i).start()
        load_wo(i).wait()
        side_wo(i).wait_recv()
        pass_wo(i).wait_recv()

    def share(i):
        weights_ready(i)
        ysend[lax.rem(i, slots)] = product(rows, rows, i).astype(BF16)
        send_y(i).start()

    def store_y(i):
        return pltpu.make_async_copy(yout.at[lax.rem(i, 2)], y_hbm.at[:, columns(i)], out_sem.at[lax.rem(i, 2)])

    def finish(i, arrived):
        value = product(0, rows, i)
        arrived()
        yout[lax.rem(i, 2)] = (value + yrecv[i].astype(F32)).astype(BF16)
        store_y(i).start()

    def share_early(i, n):
        at = slice(0, FIRST) if n == 0 else slice(FIRST, rows)
        ysend[i, at] = product(rows + at.start, at.stop - at.start, i).astype(BF16)
        send_early(i, n).start()

    with jax.named_scope("early_0"):
        weights_ready(0)
        share_early(0, 0)
    with jax.named_scope("last_rows"):
        send_x[3].wait_recv()
        norm(rows + FIRST, rows - FIRST)
        queries(0, 8, 7, 1, step=ROWS)
    with jax.named_scope("early_1"):
        weights_ready(1)
        share_early(1, 0)
    with jax.named_scope("last_attention"):
        attention(0, 4, 7, 1)
    with jax.named_scope("early_2"):
        weights_ready(2)
        share_early(2, 0)
        for i in range(EARLY):
            share_early(i, 1)
        share(3)
    with jax.named_scope("own_rest"):
        queries(5, 1, 0, 2)
        queries(7, 1, 0, 2)
        attention(3, 1, 0, 4)
    with jax.named_scope("finish_early"):
        for i in range(EARLY):
            if i == 2:
                store_y(0).wait()
            finish(i, lambda i=i: arrive([send_early(i, 0), send_early(i, 1)]))

    def step(i, _):
        @pl.when((i >= slots) & (i < slots + EARLY))
        def _():
            for n in range(2):
                send_early_at(i - slots, n).wait_send()

        @pl.when(i >= slots + EARLY)
        def _():
            send_y(i - slots).wait_send()

        share(i)
        store_y(i - 3).wait()
        finish(i - 1, send_y(i - 1).wait_recv)
        return 0

    def send_early_at(i, n):
        at = slice(0, FIRST) if n == 0 else slice(FIRST, rows)
        return copies.make(ysend.at[i, at], yrecv.at[i, at], y_early + 2 * i + n, over_x)

    with jax.named_scope("y_loop"):
        lax.fori_loop(EARLY + 1, pieces, step, 0)
    with jax.named_scope("y_last"):
        store_y(pieces - 3).wait()
        finish(pieces - 1, send_y(pieces - 1).wait_recv)

    for copy in send_x + [send_a0, send_a1, pass_a] + send_b + pass_b + send_s + kv_x + kv_y + kv_d + sum(kv_s, []):
        copy.wait_send()

    def sent(i):
        send_wo(i).wait_send()
        side_wo(i).wait_send()
        pass_wo(i).wait_send()

        @pl.when(i >= pieces - slots)
        def _():
            send_y(i).wait_send()

    each(sent)
    for copy in keep:
        copy.wait()
    store_y(pieces - 2).wait()
    store_y(pieces - 1).wait()


def settle_kernel(*refs):
    for src, dst in zip(refs[:3], refs[3:]):
        dst[...] = src[...]


def settle(arrays, steps=8):
    specs = [pl.BlockSpec((a.shape[0] // steps, a.shape[1]), lambda i: (i, 0)) for a in arrays]
    return pl.pallas_call(
        settle_kernel,
        grid=(steps,),
        in_specs=specs,
        out_specs=specs,
        out_shape=[jax.ShapeDtypeStruct(a.shape, a.dtype) for a in arrays],
        name="settle",
    )(*arrays)


def solution(mesh):
    def local_step(x_loc, ln_gain, wq_loc, w_kv, wo_loc, positions):
        rows, width = x_loc.shape
        keys = positions.shape[0]
        depth = w_kv.shape[1] // 2
        pieces = 16
        part = width // pieces

        whole = pl.BlockSpec(memory_space=pl.ANY)
        vmem = pl.BlockSpec(memory_space=pltpu.VMEM)
        heads = 8
        outs = pl.pallas_call(
            kernel,
            out_shape=[
                jax.ShapeDtypeStruct((rows, width), BF16),
                jax.ShapeDtypeStruct((keys, depth), BF16),
                jax.ShapeDtypeStruct((keys, depth), BF16),
            ],
            in_specs=[whole] * 4 + [vmem] * 3,
            out_specs=[whole] * 3,
            scratch_shapes=[
                pltpu.VMEM((2 * rows, width), BF16),
                pltpu.VMEM((keys, depth), BF16),
                pltpu.VMEM((keys, depth), BF16),
                pltpu.VMEM((heads, width, depth), BF16),
                pltpu.VMEM((4, pieces, 2 * depth, part), BF16),
                pltpu.VMEM((2 * rows, heads * depth), BF16),
                pltpu.VMEM((2, BLOCK, KEYS), F32),
                pltpu.VMEM((8, rows, part), BF16),
                pltpu.VMEM((pieces, rows, part), BF16),
                pltpu.VMEM((2, rows, part), BF16),
                pltpu.VMEM((2 * rows, 128), jnp.int32),
                pltpu.SemaphoreType.DMA((N_COPIES,)),
                pltpu.SemaphoreType.DMA((N_COPIES,)),
                pltpu.SemaphoreType.DMA((24,)),
                pltpu.SemaphoreType.DMA((4,)),
            ],
            compiler_params=pltpu.CompilerParams(collective_id=0, has_side_effects=True, vmem_limit_bytes=VMEM_LIMIT),
            name="layer",
        )(x_loc, wq_loc, w_kv, wo_loc, ln_gain.reshape(1, width), positions.reshape(keys // 128, 128), positions.reshape(1, keys))
        return tuple(settle(outs))

    return jax.shard_map(
        local_step,
        mesh=mesh,
        in_specs=(P("model", None), P(None), P(None, "model"), P(None, None), P("model", None), P(None)),
        out_specs=(P("model", None), P(None, None), P(None, None)),
        check_vma=False,
    )
```

```python
import functools
import math

import jax
import jax.numpy as jnp
from jax import lax
from jax.experimental import pallas as pl
from jax.experimental.pallas import tpu as pltpu
from jax.sharding import PartitionSpec as P

NORM_EPS = 1e-6
NEG = -1e30
F32 = jnp.float32
BF16 = jnp.bfloat16
MESH = pl.DeviceIdType.MESH
VMEM_LIMIT = 67_000_000

BLOCK = 256
ROWS = 128
KEYS = 1024
X_CUT = (0, 64, 256, 384, 512)
A_CUT = 1024
B_CUT = 3072
FIRST = 384
EARLY = 3


class Copies:
    def __init__(self, send, recv):
        self.send, self.recv, self.used = send, recv, 0

    def take(self, n=1):
        first = self.used
        self.used += n
        return first

    def make(self, src, dst, i, peer):
        return pltpu.make_async_remote_copy(
            src_ref=src, dst_ref=dst, send_sem=self.send.at[i], recv_sem=self.recv.at[i], device_id=(peer,), device_id_type=MESH
        )


N_COPIES = 97


def kernel(
    x_hbm, wq_hbm, wkv_hbm, wo_hbm, gain_ref, pos_ref, pk_ref,
    y_hbm, k_hbm, v_hbm,
    h, kbuf, vbuf, wq, wo, o, s, ysend, yrecv, yout, pq_ref,
    send, recv, local, out_sem,
):
    me = lax.axis_index("model")
    rows = x_hbm.shape[0]
    width = x_hbm.shape[1]
    depth = kbuf.shape[1]
    keys = kbuf.shape[0]
    pieces = wo.shape[1]
    part = width // pieces
    slots = ysend.shape[0]

    def flip(bit):
        return me + bit - 2 * bit * lax.rem(lax.div(me, bit), 2)

    side, over_x, over_y = flip(1), flip(2), flip(4)
    over_d = over_x + over_y - me
    copies = Copies(send, recv)

    half = rows // 2
    load_x = [pltpu.make_async_copy(x_hbm.at[i * half : (i + 1) * half], h.at[i * half : (i + 1) * half], local.at[i]) for i in range(2)]
    quarter = width // 4
    load_kv = [
        pltpu.make_async_copy(wkv_hbm.at[j * quarter : (j + 1) * quarter], o.at[:, j * 2 * depth : (j + 1) * 2 * depth], local.at[2 + j])
        for j in range(4)
    ]
    load_wq = [pltpu.make_async_copy(wq_hbm.at[:, i * depth : (i + 1) * depth], wq.at[i], local.at[6 + i]) for i in range(2)]
    for copy in load_x + load_kv:
        copy.start()

    barrier = pltpu.get_barrier_semaphore()
    for peer in (side, over_x, over_y):
        pl.semaphore_signal(barrier, inc=1, device_id=(peer,), device_id_type=MESH)
    pl.semaphore_wait(barrier, 3)

    send_x = []
    for a, b in zip(X_CUT, X_CUT[1:]):
        send_x.append(copies.make(x_hbm.at[a:b], h.at[rows + a : rows + b], copies.take(), over_x))
    send_a0 = copies.make(wq_hbm.at[0:A_CUT, 0:depth], wq.at[4, 0:A_CUT], copies.take(), over_y)
    send_a1 = copies.make(wq_hbm.at[A_CUT:width, 0:depth], wq.at[4, A_CUT:width], copies.take(), over_y)
    b_cuts = ((0, B_CUT), (B_CUT, width))
    send_b = [copies.make(wq_hbm.at[a:b, depth : 2 * depth], wq.at[5, a:b], copies.take(), over_y) for a, b in b_cuts]
    send_s = [copies.make(wq_hbm.at[:, i * depth : (i + 1) * depth], wq.at[2 + i], copies.take(), side) for i in range(2)]
    pass_a = copies.make(wq.at[4], wq.at[6], copies.take(), side)
    pass_b = [copies.make(wq.at[5, a:b], wq.at[7, a:b], copies.take(), side) for a, b in b_cuts]

    def block(buf, owner):
        return buf.at[pl.ds(pl.multiple_of(owner * rows, rows), rows)]

    def send_block(owner, peer):
        return [copies.make(block(buf, owner), block(buf, owner), copies.take(), peer) for buf in (kbuf, vbuf)]

    kv_x, kv_y = send_block(me, over_x), send_block(me, over_y)
    kv_d = send_block(over_y, over_x)
    kv_s = [send_block(owner, side) for owner in (me, over_x, over_y, over_d)]
    wo_first = copies.take(pieces)
    wo_side_first = copies.take(pieces)
    wo_pass_first = copies.take(pieces)
    y_first = copies.take(pieces)
    y_early = copies.take(2 * EARLY)

    def columns(i):
        return pl.ds(pl.multiple_of(i * part, part), part)

    def send_wo(i):
        return copies.make(wo_hbm.at[:, columns(i)], wo.at[2, i], wo_first + i, over_y)

    def side_wo(i):
        return copies.make(wo_hbm.at[:, columns(i)], wo.at[1, i], wo_side_first + i, side)

    def pass_wo(i):
        return copies.make(wo.at[2, i], wo.at[3, i], wo_pass_first + i, side)

    def send_y(i):
        return copies.make(ysend.at[lax.rem(i, slots)], yrecv.at[i], y_first + i, over_x)

    def start(group):
        for copy in group:
            copy.start()

    def arrive(group):
        for copy in group:
            copy.wait_recv()

    assert copies.used == N_COPIES

    send_x[0].start()
    send_a0.start()
    start(send_s)
    start(load_wq)

    def load_wo(i):
        return pltpu.make_async_copy(wo_hbm.at[:, columns(i)], wo.at[0, i], local.at[8 + i])

    gain = gain_ref[...]

    def norm(row0, count, step=32):
        def body(i, _):
            at = pl.ds(pl.multiple_of(row0 + i * step, step), step)
            x = h[at, :].astype(F32)
            mean = jnp.sum(x, axis=1, keepdims=True) * (1.0 / width)
            x = x - mean
            var = jnp.sum(x * x, axis=1, keepdims=True) * (1.0 / width)
            h[at, :] = (x * lax.rsqrt(var + NORM_EPS) * gain).astype(BF16)
            return 0

        lax.fori_loop(0, count // step, body, 0)

    for i in range(2):
        load_x[i].wait()
    norm(0, rows)
    for copy in load_kv:
        copy.wait()

    def keys_values(i, _):
        at = pl.ds(pl.multiple_of(i * BLOCK, BLOCK), BLOCK)
        acc = None
        for j in range(4):
            dot = jnp.dot(
                h[at, j * quarter : (j + 1) * quarter], o[:, j * 2 * depth : (j + 1) * 2 * depth], preferred_element_type=F32
            )
            acc = dot if acc is None else acc + dot
        to = pl.ds(pl.multiple_of(me * rows + i * BLOCK, BLOCK), BLOCK)
        kbuf[to, :] = acc[:, :depth].astype(BF16)
        vbuf[to, :] = acc[:, depth:].astype(BF16)
        return 0

    lax.fori_loop(0, rows // BLOCK, keys_values, 0)
    start(kv_x)
    start(kv_y)
    start(kv_s[0])

    def queries(head0, heads, block0, blocks, step=BLOCK, skip=8):
        def body(t, _):
            head = head0 + lax.div(t, blocks)
            head = head + lax.div(head, skip)
            row = pl.multiple_of((block0 + lax.rem(t, blocks)) * step, step)
            col = pl.multiple_of(head * depth, depth)
            q = jnp.dot(h[pl.ds(row, step), :], wq[head], preferred_element_type=F32)
            o[pl.ds(row, step), pl.ds(col, depth)] = q.astype(BF16)
            return 0

        lax.fori_loop(0, heads * blocks, body, 0)

    factor = depth ** -0.5 * math.log2(math.e)

    def attention(pair0, pairs, block0, blocks):
        def body(t, _):
            pair = pair0 + lax.div(t, blocks)
            head = 2 * pair - lax.div(pair, 3)
            other = head + 1 + lax.div(pair, 2)
            at = pl.ds(pl.multiple_of((block0 + lax.rem(t, blocks)) * ROWS, ROWS), ROWS)
            one = pl.ds(pl.multiple_of(head * depth, depth), depth)
            two = pl.ds(pl.multiple_of(other * depth, depth), depth)
            q = jnp.concatenate([o[at, one], o[at, two]], axis=0)
            row_pos = pq_ref[at, 0:1]
            row_pos = jnp.concatenate([row_pos, row_pos], axis=0)

            def scores(j):
                lo = j * KEYS
                dot = lax.dot_general(q, kbuf[lo : lo + KEYS, :], (((1,), (1,)), ((), ())), preferred_element_type=F32)
                dot = jnp.where(pk_ref[:, lo : lo + KEYS] <= row_pos, dot, NEG)
                s[j % 2] = dot
                return jnp.max(dot, axis=1, keepdims=True)

            steps = keys // KEYS
            top = scores(0)
            best = total = acc = None
            for j in range(steps):
                after = scores(j + 1) if j + 1 < steps else None
                new = jnp.maximum(best, top) if j else top
                p = jnp.exp2((s[j % 2] - new) * factor)
                sums = jnp.sum(p, axis=1, keepdims=True)
                pv = jnp.dot(p.astype(BF16), vbuf[j * KEYS : (j + 1) * KEYS, :], preferred_element_type=F32)
                if j:
                    scale = jnp.exp2((best - new) * factor)
                    total = total * scale + sums
                    acc = acc * scale + pv
                else:
                    total, acc = sums, pv
                best, top = new, after
            acc = (acc * (1.0 / total)).astype(BF16)
            o[at, one] = acc[:ROWS]
            o[at, two] = acc[ROWS:]
            return 0

        lax.fori_loop(0, pairs * blocks, body, 0)

    lanes = pq_ref.shape[1]
    for n, device in enumerate((me, over_x)):
        for b in range(rows // lanes):
            line = pos_ref[pl.ds(device * (rows // lanes) + b, 1), :]
            first = n * rows + b * lanes
            pq_ref[first : first + lanes, :] = jnp.broadcast_to(line, (lanes, lanes)).T

    def each(body, first=0, end=None):
        def step(i, _):
            body(i)
            return 0

        lax.fori_loop(first, pieces if end is None else end, step, 0)

    for copy in load_wq:
        copy.wait()
    queries(0, 2, 0, 2)
    start([send_a1] + send_b)
    each(lambda i: send_wo(i).start())
    arrive(kv_y)
    start(kv_d)
    start(send_x[1:])
    start(kv_s[2])
    arrive(kv_x)
    start(kv_s[1])
    arrive(send_s)
    queries(2, 2, 0, 2)
    arrive(kv_d)
    start(kv_s[3])
    each(lambda i: side_wo(i).start())
    each(lambda i: load_wo(i).start())
    for group in kv_s:
        arrive(group)
    keep = [pltpu.make_async_copy(kbuf, k_hbm, out_sem.at[2]), pltpu.make_async_copy(vbuf, v_hbm, out_sem.at[3])]
    start(keep)

    attention(0, 2, 0, 4)
    arrive([send_a0, send_a1])
    pass_a.start()
    queries(4, 1, 0, 2)
    pass_a.wait_recv()
    queries(6, 1, 0, 2)
    attention(2, 1, 0, 4)
    arrive(send_x[:2])
    norm(rows, 256)
    queries(0, 6, 2, 1, skip=5)
    attention(0, 3, 4, 2)
    send_x[2].wait_recv()
    norm(rows + 256, 128)
    queries(0, 6, 6, 1, step=ROWS, skip=5)
    attention(0, 3, 6, 1)
    send_b[0].wait_recv()
    pass_b[0].start()
    send_b[1].wait_recv()
    pass_b[1].start()
    queries(5, 1, 4, 3, step=ROWS)
    arrive(pass_b)
    queries(7, 1, 4, 3, step=ROWS)
    attention(3, 1, 4, 3)

    def product(row0, count, i):
        acc = None
        for b in range(4):
            dot = jnp.dot(o[row0 : row0 + count, b * 2 * depth : (b + 1) * 2 * depth], wo[b, i], preferred_element_type=F32)
            acc = dot if acc is None else acc + dot
        return acc

    def weights_ready(i):
        send_wo(i).wait_recv()
        pass_wo(i).start()
        load_wo(i).wait()
        side_wo(i).wait_recv()
        pass_wo(i).wait_recv()

    def share(i):
        weights_ready(i)
        ysend[lax.rem(i, slots)] = product(rows, rows, i).astype(BF16)
        send_y(i).start()

    def store_y(i):
        return pltpu.make_async_copy(yout.at[lax.rem(i, 2)], y_hbm.at[:, columns(i)], out_sem.at[lax.rem(i, 2)])

    def early_part(n):
        return slice(0, FIRST) if n == 0 else slice(FIRST, rows)

    def send_early(i, n):
        at = early_part(n)
        return copies.make(ysend.at[i, at], yrecv.at[i, at], y_early + 2 * i + n, over_x)

    def share_early(i, n):
        at = early_part(n)
        ysend[i, at] = product(rows + at.start, at.stop - at.start, i).astype(BF16)
        send_early(i, n).start()

    def finish(i):
        value = product(0, rows, i)

        @pl.when(i < EARLY)
        def _():
            for n in range(2):
                send_early(i, n).wait_recv()

        @pl.when(i >= EARLY)
        def _():
            send_y(i).wait_recv()

        @pl.when(i >= 2)
        def _():
            store_y(i - 2).wait()

        yout[lax.rem(i, 2)] = (value + yrecv[i].astype(F32)).astype(BF16)
        store_y(i).start()

    weights_ready(0)
    share_early(0, 0)
    send_x[3].wait_recv()
    norm(rows + FIRST, rows - FIRST)
    queries(0, 8, 7, 1, step=ROWS)
    weights_ready(1)
    share_early(1, 0)
    attention(0, 2, 7, 1)
    weights_ready(2)
    share_early(2, 0)
    attention(2, 2, 7, 1)
    for i in range(EARLY):
        share_early(i, 1)
    share(3)
    queries(5, 1, 0, 2)
    queries(7, 1, 0, 2)
    share(4)
    attention(3, 1, 0, 2)
    share(5)
    attention(3, 1, 2, 2)
    ahead = 6
    lag = 4

    def step(i, _):
        @pl.when(i < pieces)
        def _():
            @pl.when((i >= slots) & (i < slots + EARLY))
            def _():
                for n in range(2):
                    send_early(i - slots, n).wait_send()

            @pl.when(i >= slots + EARLY)
            def _():
                send_y(i - slots).wait_send()

            share(i)

        finish(i - lag)
        return 0

    def catch_up(i, _):
        finish(i)
        return 0

    lax.fori_loop(0, ahead - lag, catch_up, 0)
    lax.fori_loop(ahead, pieces + lag, step, 0)

    for copy in send_x + [send_a0, send_a1, pass_a] + send_b + pass_b + send_s + kv_x + kv_y + kv_d + sum(kv_s, []):
        copy.wait_send()

    def sent(i):
        send_wo(i).wait_send()
        side_wo(i).wait_send()
        pass_wo(i).wait_send()

        @pl.when(i >= pieces - slots)
        def _():
            send_y(i).wait_send()

    each(sent)
    for copy in keep:
        copy.wait()
    store_y(pieces - 2).wait()
    store_y(pieces - 1).wait()


def settle_kernel(n, *refs):
    srcs, dsts, bufs, read, write = refs[:3], refs[3:6], refs[6:9], refs[9], refs[10]

    def pieces():
        for a, (src, dst, buf) in enumerate(zip(srcs, dsts, bufs)):
            size = src.shape[0] // n
            for i in range(n):
                at = slice(i * size, (i + 1) * size)
                yield (
                    pltpu.make_async_copy(src.at[at], buf.at[at], read.at[a * n + i]),
                    pltpu.make_async_copy(buf.at[at], dst.at[at], write.at[a * n + i]),
                )

    todo = list(pieces())
    for get, _ in todo:
        get.start()
    for get, put in todo:
        get.wait()
        put.start()
    for _, put in todo:
        put.wait()


def settle(arrays, n=4):
    whole = pl.BlockSpec(memory_space=pl.ANY)
    return pl.pallas_call(
        functools.partial(settle_kernel, n),
        in_specs=[whole] * 3,
        out_specs=[whole] * 3,
        out_shape=[jax.ShapeDtypeStruct(a.shape, a.dtype) for a in arrays],
        scratch_shapes=[pltpu.VMEM(a.shape, a.dtype) for a in arrays]
        + [pltpu.SemaphoreType.DMA((3 * n,)), pltpu.SemaphoreType.DMA((3 * n,))],
        name="settle",
    )(*arrays)


def solution(mesh):
    def local_step(x_loc, ln_gain, wq_loc, w_kv, wo_loc, positions):
        rows, width = x_loc.shape
        keys = positions.shape[0]
        depth = w_kv.shape[1] // 2
        pieces = 16
        part = width // pieces

        whole = pl.BlockSpec(memory_space=pl.ANY)
        vmem = pl.BlockSpec(memory_space=pltpu.VMEM)
        heads = 8
        outs = pl.pallas_call(
            kernel,
            out_shape=[
                jax.ShapeDtypeStruct((rows, width), BF16),
                jax.ShapeDtypeStruct((keys, depth), BF16),
                jax.ShapeDtypeStruct((keys, depth), BF16),
            ],
            in_specs=[whole] * 4 + [vmem] * 3,
            out_specs=[whole] * 3,
            scratch_shapes=[
                pltpu.VMEM((2 * rows, width), BF16),
                pltpu.VMEM((keys, depth), BF16),
                pltpu.VMEM((keys, depth), BF16),
                pltpu.VMEM((heads, width, depth), BF16),
                pltpu.VMEM((4, pieces, 2 * depth, part), BF16),
                pltpu.VMEM((2 * rows, heads * depth), BF16),
                pltpu.VMEM((2, BLOCK, KEYS), F32),
                pltpu.VMEM((8, rows, part), BF16),
                pltpu.VMEM((pieces, rows, part), BF16),
                pltpu.VMEM((2, rows, part), BF16),
                pltpu.VMEM((2 * rows, 128), jnp.int32),
                pltpu.SemaphoreType.DMA((N_COPIES,)),
                pltpu.SemaphoreType.DMA((N_COPIES,)),
                pltpu.SemaphoreType.DMA((24,)),
                pltpu.SemaphoreType.DMA((4,)),
            ],
            compiler_params=pltpu.CompilerParams(collective_id=0, has_side_effects=True, vmem_limit_bytes=VMEM_LIMIT),
            name="layer",
        )(x_loc, wq_loc, w_kv, wo_loc, ln_gain.reshape(1, width), positions.reshape(keys // 128, 128), positions.reshape(1, keys))
        return tuple(settle(outs))

    return jax.shard_map(
        local_step,
        mesh=mesh,
        in_specs=(P("model", None), P(None), P(None, "model"), P(None, None), P("model", None), P(None)),
        out_specs=(P("model", None), P(None, None), P(None, None)),
        check_vma=False,
    )
```

```python
import functools
import math

import jax
import jax.numpy as jnp
from jax import lax
from jax.experimental import pallas as pl
from jax.experimental.pallas import tpu as pltpu
from jax.sharding import PartitionSpec as P

NORM_EPS = 1e-6
NEG = -1e30
F32 = jnp.float32
BF16 = jnp.bfloat16
MESH = pl.DeviceIdType.MESH
VMEM_LIMIT = 67_000_000

BLOCK = 256
ROWS = 128
KEYS = 1024
X_CUT = (0, 64, 96, 256, 384, 512)
A_CUT = 1024
B_CUT = 3072
FIRST = 384
EARLY = 3


class Copies:
    def __init__(self, send, recv):
        self.send, self.recv, self.used = send, recv, 0

    def take(self, n=1):
        first = self.used
        self.used += n
        return first

    def make(self, src, dst, i, peer):
        return pltpu.make_async_remote_copy(
            src_ref=src, dst_ref=dst, send_sem=self.send.at[i], recv_sem=self.recv.at[i], device_id=(peer,), device_id_type=MESH
        )


N_COPIES = 98


def kernel(
    x_hbm, wq_hbm, wkv_hbm, wo_hbm, gain_ref, pos_ref, pk_ref,
    y_hbm, k_hbm, v_hbm,
    h, kbuf, vbuf, wq, wo, o, s, ysend, yrecv, yout, pq_ref,
    send, recv, local, out_sem,
):
    me = lax.axis_index("model")
    rows = x_hbm.shape[0]
    width = x_hbm.shape[1]
    depth = kbuf.shape[1]
    keys = kbuf.shape[0]
    pieces = wo.shape[1]
    part = width // pieces
    slots = ysend.shape[0]

    def flip(bit):
        return me + bit - 2 * bit * lax.rem(lax.div(me, bit), 2)

    side, over_x, over_y = flip(1), flip(2), flip(4)
    over_d = over_x + over_y - me
    copies = Copies(send, recv)

    half = rows // 2
    load_x = [pltpu.make_async_copy(x_hbm.at[i * half : (i + 1) * half], h.at[i * half : (i + 1) * half], local.at[i]) for i in range(2)]
    quarter = width // 4
    load_kv = [
        pltpu.make_async_copy(wkv_hbm.at[j * quarter : (j + 1) * quarter], o.at[:, j * 2 * depth : (j + 1) * 2 * depth], local.at[2 + j])
        for j in range(4)
    ]
    load_wq = [pltpu.make_async_copy(wq_hbm.at[:, i * depth : (i + 1) * depth], wq.at[i], local.at[6 + i]) for i in range(2)]
    for copy in load_x + load_kv:
        copy.start()

    barrier = pltpu.get_barrier_semaphore()
    for peer in (side, over_x, over_y):
        pl.semaphore_signal(barrier, inc=1, device_id=(peer,), device_id_type=MESH)
    pl.semaphore_wait(barrier, 3)

    send_x = []
    for a, b in zip(X_CUT, X_CUT[1:]):
        send_x.append(copies.make(x_hbm.at[a:b], h.at[rows + a : rows + b], copies.take(), over_x))
    send_a0 = copies.make(wq_hbm.at[0:A_CUT, 0:depth], wq.at[4, 0:A_CUT], copies.take(), over_y)
    send_a1 = copies.make(wq_hbm.at[A_CUT:width, 0:depth], wq.at[4, A_CUT:width], copies.take(), over_y)
    b_cuts = ((0, B_CUT), (B_CUT, width))
    send_b = [copies.make(wq_hbm.at[a:b, depth : 2 * depth], wq.at[5, a:b], copies.take(), over_y) for a, b in b_cuts]
    send_s = [copies.make(wq_hbm.at[:, i * depth : (i + 1) * depth], wq.at[2 + i], copies.take(), side) for i in range(2)]
    pass_a = copies.make(wq.at[4], wq.at[6], copies.take(), side)
    pass_b = [copies.make(wq.at[5, a:b], wq.at[7, a:b], copies.take(), side) for a, b in b_cuts]

    def block(buf, owner):
        return buf.at[pl.ds(pl.multiple_of(owner * rows, rows), rows)]

    def send_block(owner, peer):
        return [copies.make(block(buf, owner), block(buf, owner), copies.take(), peer) for buf in (kbuf, vbuf)]

    kv_x, kv_y = send_block(me, over_x), send_block(me, over_y)
    kv_d = send_block(over_y, over_x)
    kv_s = [send_block(owner, side) for owner in (me, over_x, over_y, over_d)]
    wo_first = copies.take(pieces)
    wo_side_first = copies.take(pieces)
    wo_pass_first = copies.take(pieces)
    y_first = copies.take(pieces)
    y_early = copies.take(2 * EARLY)

    def columns(i):
        return pl.ds(pl.multiple_of(i * part, part), part)

    def send_wo(i):
        return copies.make(wo_hbm.at[:, columns(i)], wo.at[2, i], wo_first + i, over_y)

    def side_wo(i):
        return copies.make(wo_hbm.at[:, columns(i)], wo.at[1, i], wo_side_first + i, side)

    def pass_wo(i):
        return copies.make(wo.at[2, i], wo.at[3, i], wo_pass_first + i, side)

    def send_y(i):
        return copies.make(ysend.at[lax.rem(i, slots)], yrecv.at[i], y_first + i, over_x)

    def start(group):
        for copy in group:
            copy.start()

    def arrive(group):
        for copy in group:
            copy.wait_recv()

    assert copies.used == N_COPIES

    send_x[0].start()
    send_a0.start()
    start(send_s)
    start(load_wq)

    def load_wo(i):
        return pltpu.make_async_copy(wo_hbm.at[:, columns(i)], wo.at[0, i], local.at[8 + i])

    gain = gain_ref[...]

    def norm(row0, count, step=32):
        def body(i, _):
            at = pl.ds(pl.multiple_of(row0 + i * step, step), step)
            x = h[at, :].astype(F32)
            mean = jnp.sum(x, axis=1, keepdims=True) * (1.0 / width)
            x = x - mean
            var = jnp.sum(x * x, axis=1, keepdims=True) * (1.0 / width)
            h[at, :] = (x * lax.rsqrt(var + NORM_EPS) * gain).astype(BF16)
            return 0

        lax.fori_loop(0, count // step, body, 0)

    for i in range(2):
        load_x[i].wait()
    norm(0, rows)
    for copy in load_kv:
        copy.wait()

    def keys_values(i, _):
        at = pl.ds(pl.multiple_of(i * BLOCK, BLOCK), BLOCK)
        acc = None
        for j in range(4):
            dot = jnp.dot(
                h[at, j * quarter : (j + 1) * quarter], o[:, j * 2 * depth : (j + 1) * 2 * depth], preferred_element_type=F32
            )
            acc = dot if acc is None else acc + dot
        to = pl.ds(pl.multiple_of(me * rows + i * BLOCK, BLOCK), BLOCK)
        kbuf[to, :] = acc[:, :depth].astype(BF16)
        vbuf[to, :] = acc[:, depth:].astype(BF16)
        return 0

    lax.fori_loop(0, rows // BLOCK, keys_values, 0)
    start(kv_x)
    send_x[1].start()
    start(kv_y)
    start(kv_s[0])

    def queries(head0, heads, block0, blocks, step=BLOCK, skip=8):
        def body(t, _):
            head = head0 + lax.div(t, blocks)
            head = head + lax.div(head, skip)
            row = pl.multiple_of((block0 + lax.rem(t, blocks)) * step, step)
            col = pl.multiple_of(head * depth, depth)
            q = jnp.dot(h[pl.ds(row, step), :], wq[head], preferred_element_type=F32)
            o[pl.ds(row, step), pl.ds(col, depth)] = q.astype(BF16)
            return 0

        lax.fori_loop(0, heads * blocks, body, 0)

    factor = depth ** -0.5 * math.log2(math.e)

    def attention(pair0, pairs, block0, blocks):
        def body(t, _):
            pair = pair0 + lax.div(t, blocks)
            head = 2 * pair - lax.div(pair, 3)
            other = head + 1 + lax.div(pair, 2)
            at = pl.ds(pl.multiple_of((block0 + lax.rem(t, blocks)) * ROWS, ROWS), ROWS)
            one = pl.ds(pl.multiple_of(head * depth, depth), depth)
            two = pl.ds(pl.multiple_of(other * depth, depth), depth)
            q = jnp.concatenate([o[at, one], o[at, two]], axis=0)
            row_pos = pq_ref[at, 0:1]
            row_pos = jnp.concatenate([row_pos, row_pos], axis=0)

            def scores(j):
                lo = j * KEYS
                dot = lax.dot_general(q, kbuf[lo : lo + KEYS, :], (((1,), (1,)), ((), ())), preferred_element_type=F32)
                dot = jnp.where(pk_ref[:, lo : lo + KEYS] <= row_pos, dot, NEG)
                s[j % 2] = dot
                return jnp.max(dot, axis=1, keepdims=True)

            steps = keys // KEYS
            top = scores(0)
            best = total = acc = None
            for j in range(steps):
                after = scores(j + 1) if j + 1 < steps else None
                new = jnp.maximum(best, top) if j else top
                p = jnp.exp2((s[j % 2] - new) * factor)
                sums = jnp.sum(p, axis=1, keepdims=True)
                pv = jnp.dot(p.astype(BF16), vbuf[j * KEYS : (j + 1) * KEYS, :], preferred_element_type=F32)
                if j:
                    scale = jnp.exp2((best - new) * factor)
                    total = total * scale + sums
                    acc = acc * scale + pv
                else:
                    total, acc = sums, pv
                best, top = new, after
            acc = (acc * (1.0 / total)).astype(BF16)
            o[at, one] = acc[:ROWS]
            o[at, two] = acc[ROWS:]
            return 0

        lax.fori_loop(0, pairs * blocks, body, 0)

    lanes = pq_ref.shape[1]
    for n, device in enumerate((me, over_x)):
        for b in range(rows // lanes):
            line = pos_ref[pl.ds(device * (rows // lanes) + b, 1), :]
            first = n * rows + b * lanes
            pq_ref[first : first + lanes, :] = jnp.broadcast_to(line, (lanes, lanes)).T

    def each(body, first=0, end=None):
        def step(i, _):
            body(i)
            return 0

        lax.fori_loop(first, pieces if end is None else end, step, 0)

    for copy in load_wq:
        copy.wait()
    queries(0, 2, 0, 2)
    start([send_a1] + send_b)
    each(lambda i: send_wo(i).start())
    arrive(kv_y)
    start(kv_d)
    start(send_x[2:])
    start(kv_s[2])
    arrive(kv_x)
    start(kv_s[1])
    arrive(send_s)
    queries(2, 2, 0, 2)
    arrive(kv_d)
    start(kv_s[3])
    each(lambda i: side_wo(i).start())
    each(lambda i: load_wo(i).start())
    for group in kv_s:
        arrive(group)
    keep = [pltpu.make_async_copy(kbuf, k_hbm, out_sem.at[2]), pltpu.make_async_copy(vbuf, v_hbm, out_sem.at[3])]
    start(keep)

    attention(0, 2, 0, 4)
    arrive([send_a0, send_a1])
    pass_a.start()
    queries(4, 1, 0, 2)
    pass_a.wait_recv()
    queries(6, 1, 0, 2)
    attention(2, 1, 0, 4)
    arrive(send_x[:3])
    norm(rows, 256)
    queries(0, 6, 2, 1, skip=5)
    attention(0, 3, 4, 2)
    send_x[3].wait_recv()
    norm(rows + 256, 128)
    queries(0, 6, 6, 1, step=ROWS, skip=5)
    attention(0, 3, 6, 1)
    send_b[0].wait_recv()
    pass_b[0].start()
    send_b[1].wait_recv()
    pass_b[1].start()
    queries(5, 1, 4, 3, step=ROWS)
    arrive(pass_b)
    queries(7, 1, 4, 3, step=ROWS)
    attention(3, 1, 4, 3)

    def product(row0, count, i):
        acc = None
        for b in range(4):
            dot = jnp.dot(o[row0 : row0 + count, b * 2 * depth : (b + 1) * 2 * depth], wo[b, i], preferred_element_type=F32)
            acc = dot if acc is None else acc + dot
        return acc

    def weights_ready(i):
        send_wo(i).wait_recv()
        pass_wo(i).start()
        load_wo(i).wait()
        side_wo(i).wait_recv()
        pass_wo(i).wait_recv()

    def share(i):
        weights_ready(i)
        ysend[lax.rem(i, slots)] = product(rows, rows, i).astype(BF16)
        send_y(i).start()

    def store_y(i):
        return pltpu.make_async_copy(yout.at[lax.rem(i, 2)], y_hbm.at[:, columns(i)], out_sem.at[lax.rem(i, 2)])

    def early_part(n):
        return slice(0, FIRST) if n == 0 else slice(FIRST, rows)

    def send_early(i, n):
        at = early_part(n)
        return copies.make(ysend.at[i, at], yrecv.at[i, at], y_early + 2 * i + n, over_x)

    def share_early(i, n):
        at = early_part(n)
        ysend[i, at] = product(rows + at.start, at.stop - at.start, i).astype(BF16)
        send_early(i, n).start()

    def finish(i):
        value = product(0, rows, i)

        @pl.when(i < EARLY)
        def _():
            for n in range(2):
                send_early(i, n).wait_recv()

        @pl.when(i >= EARLY)
        def _():
            send_y(i).wait_recv()

        @pl.when(i >= 2)
        def _():
            store_y(i - 2).wait()

        yout[lax.rem(i, 2)] = (value + yrecv[i].astype(F32)).astype(BF16)
        store_y(i).start()

    weights_ready(0)
    share_early(0, 0)
    send_x[4].wait_recv()
    norm(rows + FIRST, rows - FIRST)
    queries(0, 8, 7, 1, step=ROWS)
    weights_ready(1)
    share_early(1, 0)
    attention(0, 2, 7, 1)
    weights_ready(2)
    share_early(2, 0)
    attention(2, 2, 7, 1)
    for i in range(EARLY):
        share_early(i, 1)
    share(3)
    queries(5, 1, 0, 2)
    queries(7, 1, 0, 2)
    share(4)
    attention(3, 1, 0, 2)
    share(5)
    attention(3, 1, 2, 2)
    ahead = 6
    lag = 4

    def step(i, _):
        @pl.when(i < pieces)
        def _():
            @pl.when((i >= slots) & (i < slots + EARLY))
            def _():
                for n in range(2):
                    send_early(i - slots, n).wait_send()

            @pl.when(i >= slots + EARLY)
            def _():
                send_y(i - slots).wait_send()

            share(i)

        finish(i - lag)
        return 0

    def catch_up(i, _):
        finish(i)
        return 0

    lax.fori_loop(0, ahead - lag, catch_up, 0)
    lax.fori_loop(ahead, pieces + lag, step, 0)

    for copy in send_x + [send_a0, send_a1, pass_a] + send_b + pass_b + send_s + kv_x + kv_y + kv_d + sum(kv_s, []):
        copy.wait_send()

    def sent(i):
        send_wo(i).wait_send()
        side_wo(i).wait_send()
        pass_wo(i).wait_send()

        @pl.when(i >= pieces - slots)
        def _():
            send_y(i).wait_send()

    each(sent)
    for copy in keep:
        copy.wait()
    store_y(pieces - 2).wait()
    store_y(pieces - 1).wait()


def settle_kernel(n, *refs):
    srcs, dsts, bufs, read, write = refs[:3], refs[3:6], refs[6:9], refs[9], refs[10]

    def pieces():
        for a, (src, dst, buf) in enumerate(zip(srcs, dsts, bufs)):
            size = src.shape[0] // n
            for i in range(n):
                at = slice(i * size, (i + 1) * size)
                yield (
                    pltpu.make_async_copy(src.at[at], buf.at[at], read.at[a * n + i]),
                    pltpu.make_async_copy(buf.at[at], dst.at[at], write.at[a * n + i]),
                )

    todo = list(pieces())
    for get, _ in todo:
        get.start()
    for get, put in todo:
        get.wait()
        put.start()
    for _, put in todo:
        put.wait()


def settle(arrays, n=4):
    whole = pl.BlockSpec(memory_space=pl.ANY)
    return pl.pallas_call(
        functools.partial(settle_kernel, n),
        in_specs=[whole] * 3,
        out_specs=[whole] * 3,
        out_shape=[jax.ShapeDtypeStruct(a.shape, a.dtype) for a in arrays],
        scratch_shapes=[pltpu.VMEM(a.shape, a.dtype) for a in arrays]
        + [pltpu.SemaphoreType.DMA((3 * n,)), pltpu.SemaphoreType.DMA((3 * n,))],
        name="settle",
    )(*arrays)


def solution(mesh):
    def local_step(x_loc, ln_gain, wq_loc, w_kv, wo_loc, positions):
        rows, width = x_loc.shape
        keys = positions.shape[0]
        depth = w_kv.shape[1] // 2
        pieces = 16
        part = width // pieces

        whole = pl.BlockSpec(memory_space=pl.ANY)
        vmem = pl.BlockSpec(memory_space=pltpu.VMEM)
        heads = 8
        outs = pl.pallas_call(
            kernel,
            out_shape=[
                jax.ShapeDtypeStruct((rows, width), BF16),
                jax.ShapeDtypeStruct((keys, depth), BF16),
                jax.ShapeDtypeStruct((keys, depth), BF16),
            ],
            in_specs=[whole] * 4 + [vmem] * 3,
            out_specs=[whole] * 3,
            scratch_shapes=[
                pltpu.VMEM((2 * rows, width), BF16),
                pltpu.VMEM((keys, depth), BF16),
                pltpu.VMEM((keys, depth), BF16),
                pltpu.VMEM((heads, width, depth), BF16),
                pltpu.VMEM((4, pieces, 2 * depth, part), BF16),
                pltpu.VMEM((2 * rows, heads * depth), BF16),
                pltpu.VMEM((2, BLOCK, KEYS), F32),
                pltpu.VMEM((8, rows, part), BF16),
                pltpu.VMEM((pieces, rows, part), BF16),
                pltpu.VMEM((2, rows, part), BF16),
                pltpu.VMEM((2 * rows, 128), jnp.int32),
                pltpu.SemaphoreType.DMA((N_COPIES,)),
                pltpu.SemaphoreType.DMA((N_COPIES,)),
                pltpu.SemaphoreType.DMA((24,)),
                pltpu.SemaphoreType.DMA((4,)),
            ],
            compiler_params=pltpu.CompilerParams(collective_id=0, has_side_effects=True, vmem_limit_bytes=VMEM_LIMIT),
            name="layer",
        )(x_loc, wq_loc, w_kv, wo_loc, ln_gain.reshape(1, width), positions.reshape(keys // 128, 128), positions.reshape(1, keys))
        return tuple(settle(outs))

    return jax.shard_map(
        local_step,
        mesh=mesh,
        in_specs=(P("model", None), P(None), P(None, "model"), P(None, None), P("model", None), P(None)),
        out_specs=(P("model", None), P(None, None), P(None, None)),
        check_vma=False,
    )
```

```python
import functools
import math

import jax
import jax.numpy as jnp
from jax import lax
from jax.experimental import pallas as pl
from jax.experimental.pallas import tpu as pltpu
from jax.sharding import PartitionSpec as P

NORM_EPS = 1e-6
NEG = -1e30
F32 = jnp.float32
BF16 = jnp.bfloat16
MESH = pl.DeviceIdType.MESH
VMEM_LIMIT = 67_000_000

BLOCK = 256
ROWS = 128
KEYS = 1024
X_CUT = (0, 64, 96, 256, 384, 512)
A_CUT = 1024
B_CUT = 3072
FIRST = 384
EARLY = 3


class Copies:
    def __init__(self, send, recv):
        self.send, self.recv, self.used = send, recv, 0

    def take(self, n=1):
        first = self.used
        self.used += n
        return first

    def make(self, src, dst, i, peer):
        return pltpu.make_async_remote_copy(
            src_ref=src, dst_ref=dst, send_sem=self.send.at[i], recv_sem=self.recv.at[i], device_id=(peer,), device_id_type=MESH
        )


N_COPIES = 98


def kernel(
    x_hbm, wq_hbm, wkv_hbm, wo_hbm, gain_ref, pos_ref, pk_ref,
    y_hbm, k_hbm, v_hbm,
    h, kbuf, vbuf, wq, wo, o, s, ysend, yrecv, yout, pq_ref,
    send, recv, local, out_sem,
):
    me = lax.axis_index("model")
    rows = x_hbm.shape[0]
    width = x_hbm.shape[1]
    depth = kbuf.shape[1]
    keys = kbuf.shape[0]
    pieces = wo.shape[1]
    part = width // pieces
    slots = ysend.shape[0]

    def flip(bit):
        return me + bit - 2 * bit * lax.rem(lax.div(me, bit), 2)

    side, over_x, over_y = flip(1), flip(2), flip(4)
    over_d = over_x + over_y - me
    copies = Copies(send, recv)

    half = rows // 2
    load_x = [pltpu.make_async_copy(x_hbm.at[i * half : (i + 1) * half], h.at[i * half : (i + 1) * half], local.at[i]) for i in range(2)]
    quarter = width // 4
    load_kv = [
        pltpu.make_async_copy(wkv_hbm.at[j * quarter : (j + 1) * quarter], o.at[:, j * 2 * depth : (j + 1) * 2 * depth], local.at[2 + j])
        for j in range(4)
    ]
    load_wq = [pltpu.make_async_copy(wq_hbm.at[:, i * depth : (i + 1) * depth], wq.at[i], local.at[6 + i]) for i in range(2)]
    for copy in load_x + load_kv:
        copy.start()

    barrier = pltpu.get_barrier_semaphore()
    for peer in (side, over_x, over_y):
        pl.semaphore_signal(barrier, inc=1, device_id=(peer,), device_id_type=MESH)
    pl.semaphore_wait(barrier, 3)

    send_x = []
    for a, b in zip(X_CUT, X_CUT[1:]):
        send_x.append(copies.make(x_hbm.at[a:b], h.at[rows + a : rows + b], copies.take(), over_x))
    send_a0 = copies.make(wq_hbm.at[0:A_CUT, 0:depth], wq.at[4, 0:A_CUT], copies.take(), over_y)
    send_a1 = copies.make(wq.at[0, A_CUT:width], wq.at[4, A_CUT:width], copies.take(), over_y)
    b_cuts = ((0, B_CUT), (B_CUT, width))
    send_b = [copies.make(wq.at[1, a:b], wq.at[5, a:b], copies.take(), over_y) for a, b in b_cuts]
    send_s = [copies.make(wq_hbm.at[:, i * depth : (i + 1) * depth], wq.at[2 + i], copies.take(), side) for i in range(2)]
    pass_a = copies.make(wq.at[4], wq.at[6], copies.take(), side)
    pass_b = [copies.make(wq.at[5, a:b], wq.at[7, a:b], copies.take(), side) for a, b in b_cuts]

    def block(buf, owner):
        return buf.at[pl.ds(pl.multiple_of(owner * rows, rows), rows)]

    def send_block(owner, peer):
        return [copies.make(block(buf, owner), block(buf, owner), copies.take(), peer) for buf in (kbuf, vbuf)]

    kv_x, kv_y = send_block(me, over_x), send_block(me, over_y)
    kv_d = send_block(over_y, over_x)
    kv_s = [send_block(owner, side) for owner in (me, over_x, over_y, over_d)]
    wo_first = copies.take(pieces)
    wo_side_first = copies.take(pieces)
    wo_pass_first = copies.take(pieces)
    y_first = copies.take(pieces)
    y_early = copies.take(2 * EARLY)

    def columns(i):
        return pl.ds(pl.multiple_of(i * part, part), part)

    def send_wo(i):
        return copies.make(wo.at[0, i], wo.at[2, i], wo_first + i, over_y)

    def side_wo(i):
        return copies.make(wo.at[0, i], wo.at[1, i], wo_side_first + i, side)

    def pass_wo(i):
        return copies.make(wo.at[2, i], wo.at[3, i], wo_pass_first + i, side)

    def send_y(i):
        return copies.make(ysend.at[lax.rem(i, slots)], yrecv.at[i], y_first + i, over_x)

    def start(group):
        for copy in group:
            copy.start()

    def arrive(group):
        for copy in group:
            copy.wait_recv()

    assert copies.used == N_COPIES

    send_x[0].start()
    send_a0.start()
    start(send_s)
    start(load_wq)

    def load_wo(i):
        return pltpu.make_async_copy(wo_hbm.at[:, columns(i)], wo.at[0, i], local.at[8 + i])

    def each(body, first=0, end=None):
        def step(i, _):
            body(i)
            return 0

        lax.fori_loop(first, pieces if end is None else end, step, 0)

    each(lambda i: load_wo(i).start())

    gain = gain_ref[...]

    def norm(row0, count, step=32):
        def body(i, _):
            at = pl.ds(pl.multiple_of(row0 + i * step, step), step)
            x = h[at, :].astype(F32)
            mean = jnp.sum(x, axis=1, keepdims=True) * (1.0 / width)
            x = x - mean
            var = jnp.sum(x * x, axis=1, keepdims=True) * (1.0 / width)
            h[at, :] = (x * lax.rsqrt(var + NORM_EPS) * gain).astype(BF16)
            return 0

        lax.fori_loop(0, count // step, body, 0)

    for i in range(2):
        load_x[i].wait()
    norm(0, rows)
    for copy in load_kv:
        copy.wait()

    def keys_values(i, _):
        at = pl.ds(pl.multiple_of(i * BLOCK, BLOCK), BLOCK)
        acc = None
        for j in range(4):
            dot = jnp.dot(
                h[at, j * quarter : (j + 1) * quarter], o[:, j * 2 * depth : (j + 1) * 2 * depth], preferred_element_type=F32
            )
            acc = dot if acc is None else acc + dot
        to = pl.ds(pl.multiple_of(me * rows + i * BLOCK, BLOCK), BLOCK)
        kbuf[to, :] = acc[:, :depth].astype(BF16)
        vbuf[to, :] = acc[:, depth:].astype(BF16)
        return 0

    lax.fori_loop(0, rows // BLOCK, keys_values, 0)
    start(kv_x)
    send_x[1].start()
    start(kv_y)
    start(kv_s[0])

    def queries(head0, heads, block0, blocks, step=BLOCK, skip=8):
        def body(t, _):
            head = head0 + lax.div(t, blocks)
            head = head + lax.div(head, skip)
            row = pl.multiple_of((block0 + lax.rem(t, blocks)) * step, step)
            col = pl.multiple_of(head * depth, depth)
            q = jnp.dot(h[pl.ds(row, step), :], wq[head], preferred_element_type=F32)
            o[pl.ds(row, step), pl.ds(col, depth)] = q.astype(BF16)
            return 0

        lax.fori_loop(0, heads * blocks, body, 0)

    factor = depth ** -0.5 * math.log2(math.e)

    def attention(pair0, pairs, block0, blocks):
        def body(t, _):
            pair = pair0 + lax.div(t, blocks)
            head = 2 * pair - lax.div(pair, 3)
            other = head + 1 + lax.div(pair, 2)
            at = pl.ds(pl.multiple_of((block0 + lax.rem(t, blocks)) * ROWS, ROWS), ROWS)
            one = pl.ds(pl.multiple_of(head * depth, depth), depth)
            two = pl.ds(pl.multiple_of(other * depth, depth), depth)
            q = jnp.concatenate([o[at, one], o[at, two]], axis=0)
            row_pos = pq_ref[at, 0:1]
            row_pos = jnp.concatenate([row_pos, row_pos], axis=0)

            def scores(j):
                lo = j * KEYS
                dot = lax.dot_general(q, kbuf[lo : lo + KEYS, :], (((1,), (1,)), ((), ())), preferred_element_type=F32)
                dot = jnp.where(pk_ref[:, lo : lo + KEYS] <= row_pos, dot, NEG)
                s[j % 2] = dot
                return jnp.max(dot, axis=1, keepdims=True)

            steps = keys // KEYS
            top = scores(0)
            best = total = acc = None
            for j in range(steps):
                after = scores(j + 1) if j + 1 < steps else None
                new = jnp.maximum(best, top) if j else top
                p = jnp.exp2((s[j % 2] - new) * factor)
                sums = jnp.sum(p, axis=1, keepdims=True)
                pv = jnp.dot(p.astype(BF16), vbuf[j * KEYS : (j + 1) * KEYS, :], preferred_element_type=F32)
                if j:
                    scale = jnp.exp2((best - new) * factor)
                    total = total * scale + sums
                    acc = acc * scale + pv
                else:
                    total, acc = sums, pv
                best, top = new, after
            acc = (acc * (1.0 / total)).astype(BF16)
            o[at, one] = acc[:ROWS]
            o[at, two] = acc[ROWS:]
            return 0

        lax.fori_loop(0, pairs * blocks, body, 0)

    lanes = pq_ref.shape[1]
    for n, device in enumerate((me, over_x)):
        for b in range(rows // lanes):
            line = pos_ref[pl.ds(device * (rows // lanes) + b, 1), :]
            first = n * rows + b * lanes
            pq_ref[first : first + lanes, :] = jnp.broadcast_to(line, (lanes, lanes)).T

    for copy in load_wq:
        copy.wait()
    queries(0, 2, 0, 2)
    start([send_a1] + send_b)
    each(lambda i: load_wo(i).wait())
    each(lambda i: send_wo(i).start())
    arrive(kv_y)
    start(kv_d)
    start(send_x[2:])
    start(kv_s[2])
    arrive(kv_x)
    start(kv_s[1])
    arrive(send_s)
    queries(2, 2, 0, 2)
    arrive(kv_d)
    start(kv_s[3])
    each(lambda i: side_wo(i).start())
    for group in kv_s:
        arrive(group)
    keep = [pltpu.make_async_copy(kbuf, k_hbm, out_sem.at[2]), pltpu.make_async_copy(vbuf, v_hbm, out_sem.at[3])]
    start(keep)

    attention(0, 2, 0, 4)
    arrive([send_a0, send_a1])
    pass_a.start()
    queries(4, 1, 0, 2)
    pass_a.wait_recv()
    queries(6, 1, 0, 2)
    attention(2, 1, 0, 4)
    arrive(send_x[:3])
    norm(rows, 256)
    queries(0, 6, 2, 1, skip=5)
    attention(0, 3, 4, 2)
    send_x[3].wait_recv()
    norm(rows + 256, 128)
    queries(0, 6, 6, 1, step=ROWS, skip=5)
    attention(0, 3, 6, 1)
    send_b[0].wait_recv()
    pass_b[0].start()
    send_b[1].wait_recv()
    pass_b[1].start()
    queries(5, 1, 4, 3, step=ROWS)
    arrive(pass_b)
    queries(7, 1, 4, 3, step=ROWS)
    attention(3, 1, 4, 3)

    def product(row0, count, i):
        acc = None
        for b in range(4):
            dot = jnp.dot(o[row0 : row0 + count, b * 2 * depth : (b + 1) * 2 * depth], wo[b, i], preferred_element_type=F32)
            acc = dot if acc is None else acc + dot
        return acc

    def weights_ready(i):
        send_wo(i).wait_recv()
        pass_wo(i).start()
        side_wo(i).wait_recv()
        pass_wo(i).wait_recv()

    def share(i):
        weights_ready(i)
        ysend[lax.rem(i, slots)] = product(rows, rows, i).astype(BF16)
        send_y(i).start()

    def store_y(i):
        return pltpu.make_async_copy(yout.at[lax.rem(i, 2)], y_hbm.at[:, columns(i)], out_sem.at[lax.rem(i, 2)])

    def early_part(n):
        return slice(0, FIRST) if n == 0 else slice(FIRST, rows)

    def send_early(i, n):
        at = early_part(n)
        return copies.make(ysend.at[i, at], yrecv.at[i, at], y_early + 2 * i + n, over_x)

    def share_early(i, n):
        at = early_part(n)
        ysend[i, at] = product(rows + at.start, at.stop - at.start, i).astype(BF16)
        send_early(i, n).start()

    def finish(i):
        value = product(0, rows, i)

        @pl.when(i < EARLY)
        def _():
            for n in range(2):
                send_early(i, n).wait_recv()

        @pl.when(i >= EARLY)
        def _():
            send_y(i).wait_recv()

        @pl.when(i >= 2)
        def _():
            store_y(i - 2).wait()

        yout[lax.rem(i, 2)] = (value + yrecv[i].astype(F32)).astype(BF16)
        store_y(i).start()

    weights_ready(0)
    share_early(0, 0)
    send_x[4].wait_recv()
    norm(rows + FIRST, rows - FIRST)
    queries(0, 8, 7, 1, step=ROWS)
    weights_ready(1)
    share_early(1, 0)
    attention(0, 2, 7, 1)
    weights_ready(2)
    share_early(2, 0)
    attention(2, 2, 7, 1)
    for i in range(EARLY):
        share_early(i, 1)
    share(3)
    queries(5, 1, 0, 2)
    queries(7, 1, 0, 2)
    share(4)
    attention(3, 1, 0, 2)
    share(5)
    attention(3, 1, 2, 2)
    ahead = 6
    lag = 4

    def step(i, _):
        @pl.when(i < pieces)
        def _():
            @pl.when((i >= slots) & (i < slots + EARLY))
            def _():
                for n in range(2):
                    send_early(i - slots, n).wait_send()

            @pl.when(i >= slots + EARLY)
            def _():
                send_y(i - slots).wait_send()

            share(i)

        finish(i - lag)
        return 0

    def catch_up(i, _):
        finish(i)
        return 0

    lax.fori_loop(0, ahead - lag, catch_up, 0)
    lax.fori_loop(ahead, pieces + lag, step, 0)

    for copy in send_x + [send_a0, send_a1, pass_a] + send_b + pass_b + send_s + kv_x + kv_y + kv_d + sum(kv_s, []):
        copy.wait_send()

    def sent(i):
        send_wo(i).wait_send()
        side_wo(i).wait_send()
        pass_wo(i).wait_send()

        @pl.when(i >= pieces - slots)
        def _():
            send_y(i).wait_send()

    each(sent)
    for copy in keep:
        copy.wait()
    store_y(pieces - 2).wait()
    store_y(pieces - 1).wait()


def settle_kernel(n, *refs):
    srcs, dsts, bufs, read, write = refs[:3], refs[3:6], refs[6:9], refs[9], refs[10]

    def pieces():
        for a, (src, dst, buf) in enumerate(zip(srcs, dsts, bufs)):
            size = src.shape[0] // n
            for i in range(n):
                at = slice(i * size, (i + 1) * size)
                yield (
                    pltpu.make_async_copy(src.at[at], buf.at[at], read.at[a * n + i]),
                    pltpu.make_async_copy(buf.at[at], dst.at[at], write.at[a * n + i]),
                )

    todo = list(pieces())
    for get, _ in todo:
        get.start()
    for get, put in todo:
        get.wait()
        put.start()
    for _, put in todo:
        put.wait()


def settle(arrays, n=4):
    whole = pl.BlockSpec(memory_space=pl.ANY)
    return pl.pallas_call(
        functools.partial(settle_kernel, n),
        in_specs=[whole] * 3,
        out_specs=[whole] * 3,
        out_shape=[jax.ShapeDtypeStruct(a.shape, a.dtype) for a in arrays],
        scratch_shapes=[pltpu.VMEM(a.shape, a.dtype) for a in arrays]
        + [pltpu.SemaphoreType.DMA((3 * n,)), pltpu.SemaphoreType.DMA((3 * n,))],
        name="settle",
    )(*arrays)


def solution(mesh):
    def local_step(x_loc, ln_gain, wq_loc, w_kv, wo_loc, positions):
        rows, width = x_loc.shape
        keys = positions.shape[0]
        depth = w_kv.shape[1] // 2
        pieces = 16
        part = width // pieces

        whole = pl.BlockSpec(memory_space=pl.ANY)
        vmem = pl.BlockSpec(memory_space=pltpu.VMEM)
        heads = 8
        outs = pl.pallas_call(
            kernel,
            out_shape=[
                jax.ShapeDtypeStruct((rows, width), BF16),
                jax.ShapeDtypeStruct((keys, depth), BF16),
                jax.ShapeDtypeStruct((keys, depth), BF16),
            ],
            in_specs=[whole] * 4 + [vmem] * 3,
            out_specs=[whole] * 3,
            scratch_shapes=[
                pltpu.VMEM((2 * rows, width), BF16),
                pltpu.VMEM((keys, depth), BF16),
                pltpu.VMEM((keys, depth), BF16),
                pltpu.VMEM((heads, width, depth), BF16),
                pltpu.VMEM((4, pieces, 2 * depth, part), BF16),
                pltpu.VMEM((2 * rows, heads * depth), BF16),
                pltpu.VMEM((2, BLOCK, KEYS), F32),
                pltpu.VMEM((8, rows, part), BF16),
                pltpu.VMEM((pieces, rows, part), BF16),
                pltpu.VMEM((2, rows, part), BF16),
                pltpu.VMEM((2 * rows, 128), jnp.int32),
                pltpu.SemaphoreType.DMA((N_COPIES,)),
                pltpu.SemaphoreType.DMA((N_COPIES,)),
                pltpu.SemaphoreType.DMA((24,)),
                pltpu.SemaphoreType.DMA((4,)),
            ],
            compiler_params=pltpu.CompilerParams(collective_id=0, has_side_effects=True, vmem_limit_bytes=VMEM_LIMIT),
            name="layer",
        )(x_loc, wq_loc, w_kv, wo_loc, ln_gain.reshape(1, width), positions.reshape(keys // 128, 128), positions.reshape(1, keys))
        return tuple(settle(outs))

    return jax.shard_map(
        local_step,
        mesh=mesh,
        in_specs=(P("model", None), P(None), P(None, "model"), P(None, None), P("model", None), P(None)),
        out_specs=(P("model", None), P(None, None), P(None, None)),
        check_vma=False,
    )
```
